32 devices in a mesh: face: 8 (over z, y), col: 4 (over x, core).
Axes of the slice: x: 2, y: 2, z: 4, core: 2. Of those that a mesh axis runs over, the one named last changes fastest.
Arguments:
- fields: float32 [4, 160, 80, 128], P(None, 'face', 'col'), may hold values from -6 to 6
- metric_diag: float32 [2, 160, 80], P(None, 'face', 'col'), may hold values from 0.05 to 0.5
- metric_cross: float32 [160, 80], P('face', 'col'), may hold values from -0.1 to 0.1
- point_mass: float32 [160, 80], P('face', 'col'), may hold values from 0.5 to 2
Outputs:
- biharmonic: float32 [4, 160, 80, 128], P(None, 'face', 'col')
The draws below stay inside these ranges and needn't reach their ends.
All inputs are finite; a program needn't handle non-finite values.
Results may differ from the reference program's by a relative error of at most 0.00024.
Values sent between devices are 32-bit elements; how exact they have to be, the bound alone decides.
A program may use at most 64 MiB of HBM per device.

```python
import math
import jax
import jax.numpy as jnp
import numpy as np
from jax import lax

FIELDS = 4
LEV = 128
NXP = 160
NYP = 80


def block_levels(key, shape, split, low, top_value):
    loudness = 1.0
    for axis_at, blocks in split:
        steps = jax.random.uniform(jax.random.fold_in(jax.random.fold_in(key, 6), axis_at), (blocks,), jnp.float32, low / len(split), top_value / len(split))
        loudness = loudness * jnp.repeat(jnp.exp(steps), shape[axis_at] // blocks).reshape((-1,) + (1,) * (len(shape) - 1 - axis_at))
    return loudness


def noise(own_key, shape, scale, bound, pieces=(), held_as=jnp.bfloat16):
    factor_of = block_levels(own_key, shape, pieces, -0.22, 0.18) if pieces else 1.0
    result = jax.random.normal(own_key, shape, jnp.float32) * scale * factor_of
    return jnp.minimum(jnp.maximum(result, -bound), bound).astype(held_as)


def setup_inputs(seed: int = 0) -> dict:
    key_list = jax.random.split(jax.random.key(seed), 5)
    fields = noise(key_list[0], (FIELDS, NXP, NYP, LEV), 1.0, 6.0, ((1, 8), (2, 4)), jnp.float32)
    metric_diag = jnp.clip(jnp.exp(math.log(0.5) - 2.3025851 * jax.random.uniform(key_list[1], (2, NXP, NYP), jnp.float32) ** block_levels(key_list[1], (2, NXP, NYP), ((1, 8), (2, 4)), -0.2, 0.2)), 0.05, 0.5)
    metric_cross = jnp.clip(jax.random.uniform(key_list[2], (NXP, NYP), jnp.float32, -0.1, 0.1) * block_levels(key_list[2], (NXP, NYP), ((0, 8), (1, 4)), -0.4, 0.0), -0.1, 0.1)
    point_mass = jnp.clip(jnp.exp(math.log(2.0) - 1.3862944 * jax.random.uniform(key_list[3], (NXP, NYP), jnp.float32) ** block_levels(key_list[3], (NXP, NYP), ((0, 8), (1, 4)), -0.2, 0.2)), 0.5, 2.0)
    return dict(fields=fields, metric_diag=metric_diag, metric_cross=metric_cross, point_mass=point_mass)


def derivative_table():
    small = 1.0 / np.sqrt(5.0)
    nodes = np.array([-1.0, -small, small, 1.0])
    count = nodes.shape[0]
    weights = np.array([np.prod([nodes[a] - nodes[k] for k in range(count) if k != a]) for a in range(count)])
    table = np.zeros((count, count))
    for a in range(count):
        for b in range(count):
            if a == b:
                table[a, b] = np.sum([1.0 / (nodes[a] - nodes[k]) for k in range(count) if k != a])
            else:
                table[a, b] = weights[a] / weights[b] / (nodes[a] - nodes[b])
    return jnp.asarray(table, jnp.float32)

def laplace(values, metric_diag, metric_cross):
    table = derivative_table()
    nfield, rows, cols, nlev = values.shape
    blocks_x = rows // 4
    blocks_y = cols // 4
    shaped = values.reshape(nfield, blocks_x, 4, blocks_y, 4, nlev)
    first_diag = metric_diag[0].reshape(1, blocks_x, 4, blocks_y, 4, 1)
    second_diag = metric_diag[1].reshape(1, blocks_x, 4, blocks_y, 4, 1)
    cross_term = metric_cross.reshape(1, blocks_x, 4, blocks_y, 4, 1)
    high = lax.Precision.HIGHEST
    grad_x = jnp.einsum('ab,febgcl->feagcl', table, shaped, precision=high)
    grad_y = jnp.einsum('cd,febgdl->febgcl', table, shaped, precision=high)
    flux_x = first_diag * grad_x + cross_term * grad_y
    flux_y = cross_term * grad_x + second_diag * grad_y
    weak = jnp.einsum('ba,febgcl->feagcl', table, flux_x, precision=high)
    weak = weak + jnp.einsum('dc,febgdl->febgcl', table, flux_y, precision=high)
    return (-weak).reshape(nfield, rows, cols, nlev)

def assemble(padded):
    rows = padded.shape[1] - 2
    cols = padded.shape[2] - 2
    row_local = jnp.arange(rows, dtype=jnp.int32) % 4
    col_local = jnp.arange(cols, dtype=jnp.int32) % 4
    row_low = (row_local == 0).astype(jnp.float32).reshape(1, rows, 1, 1)
    row_high = (row_local == 3).astype(jnp.float32).reshape(1, rows, 1, 1)
    col_low = (col_local == 0).astype(jnp.float32).reshape(1, 1, cols, 1)
    col_high = (col_local == 3).astype(jnp.float32).reshape(1, 1, cols, 1)
    summed = padded[:, 1:-1] + row_low * padded[:, :-2] + row_high * padded[:, 2:]
    return summed[:, :, 1:-1] + col_low * summed[:, :, :-2] + col_high * summed[:, :, 2:]

def wrap_pad(values):
    return jnp.pad(values, ((0, 0), (1, 1), (1, 1), (0, 0)), mode='wrap')

def reference(fields, metric_diag, metric_cross, point_mass):
    mass_sum = assemble(wrap_pad(point_mass[None, :, :, None]))
    first = assemble(wrap_pad(laplace(fields, metric_diag, metric_cross))) / mass_sum
    return assemble(wrap_pad(laplace(first, metric_diag, metric_cross))) / mass_sum
```

```python
import functools

import jax
import jax.numpy as jnp
import numpy as np
from jax import lax
from jax.experimental import pallas as pl
from jax.experimental.pallas import tpu as pltpu
from jax.sharding import PartitionSpec as P

MESH = pl.DeviceIdType.MESH


def derivative_table():
    small = 1.0 / np.sqrt(5.0)
    nodes = np.array([-1.0, -small, small, 1.0])
    count = nodes.shape[0]
    weights = np.array(
        [np.prod([nodes[a] - nodes[k] for k in range(count) if k != a]) for a in range(count)]
    )
    table = np.zeros((count, count))
    for a in range(count):
        for b in range(count):
            if a == b:
                table[a, b] = np.sum([1.0 / (nodes[a] - nodes[k]) for k in range(count) if k != a])
            else:
                table[a, b] = weights[a] / weights[b] / (nodes[a] - nodes[b])
    return [[float(np.float32(v)) for v in row] for row in table]


def dot4(coefs, terms):
    total = None
    for c, t in zip(coefs, terms):
        if isinstance(c, float) and c == 0.0:
            continue
        total = c * t if total is None else total + c * t
    return total


def kernel(
    faces, cols, nf, nbx, nby,
    fields_hbm, diag_hbm, cross_hbm, mass_hbm, out_ref,
    diag_ref, cross_ref, mass_ref, raw, U, M, W, T, spread, rM,
    sC1, rR1, rC1, rK1, sC2, rR2, rC2, rK2,
    small_sem, load_sem, mass_send, mass_recv, send_sem, recv_sem,
):
    face, col = lax.axis_index("face"), lax.axis_index("col")
    fside = (lax.rem(face + faces - 1, faces), lax.rem(face + 1, faces))
    cside = (lax.rem(col + cols - 1, cols), lax.rem(col + 1, cols))
    peers = [(fside[0], col), (fside[1], col), (face, cside[0]), (face, cside[1])]
    peers += [(fside[s], cside[t]) for s in range(2) for t in range(2)]
    opposite = [1, 0, 3, 2, 7, 6, 5, 4]

    nx, ny, nq = 4 * nbx, 4 * nby, 2 * nby
    lanes = raw.shape[-1]
    barrier = pltpu.get_barrier_semaphore()
    for peer in peers:
        pl.semaphore_signal(barrier, inc=1, device_id=peer, device_id_type=MESH)

    order = [0, nbx - 1] + list(range(1, nbx - 1))
    loads = {
        ex: pltpu.make_async_copy(
            fields_hbm.at[pl.ds(4 * ex, 4)], raw.at[pl.ds(4 * ex, 4)], load_sem.at[ex]
        )
        for ex in order
    }
    small = [
        pltpu.make_async_copy(src, dst, small_sem.at[k])
        for k, (src, dst) in enumerate(
            ((diag_hbm, diag_ref), (cross_hbm, cross_ref), (mass_hbm, mass_ref))
        )
    ]
    for copy in small:
        copy.start()
    for ex in order:
        loads[ex].start()
    for copy in small:
        copy.wait()

    D = derivative_table()
    sub = lax.broadcasted_iota(jnp.int32, (2 * nf, lanes), 0)
    is_low = sub < nf
    low = jnp.where(is_low, 1.0, 0.0)
    high = 1.0 - low

    def swap(v):
        return pltpu.roll(v, nf, 0)

    def halves(table):
        return [
            [
                jnp.where(is_low, table[2 * p][2 * q + k], table[2 * p + 1][2 * q + 1 - k])
                for q in range(2) for k in range(2)
            ]
            for p in range(2)
        ]

    minus_t = [[-D[b][a] for b in range(4)] for a in range(4)]
    D_half, minus_half = halves(D), halves(minus_t)

    row = lax.broadcasted_iota(jnp.int32, (nf * ny, 3 * ny), 0)
    lane = lax.broadcasted_iota(jnp.int32, (nf * ny, 3 * ny), 1)
    keep = jnp.zeros((nf * ny, 3 * ny), jnp.float32)
    for k in range(3):
        first_row = nf * (lane - k * ny)
        keep = jnp.where((row >= first_row) & (row < first_row + nf), 1.0, keep)
    ones = jnp.ones((3 * ny, lanes), jnp.bfloat16)

    def split(slot, m):
        parts = []
        for _ in range(3):
            part = m.astype(jnp.bfloat16).astype(jnp.float32)
            m = m - part
            parts.append(part)
        spread[slot] = jnp.concatenate(parts, axis=1)

    def spread_row(slot, x):
        left = (keep * spread[slot, pl.ds(x, 1), :]).astype(jnp.bfloat16)
        wide = jnp.dot(left, ones, preferred_element_type=jnp.float32)
        M[slot, x] = wide.reshape(nq, 2 * nf, lanes)

    split(0, diag_ref[:, 0, :])
    split(1, cross_ref[...])
    split(2, diag_ref[:, 1, :])
    for x in range(nx):
        for slot in range(3):
            spread_row(slot, x)

    def laplace(src, ex, ey):
        u = [[src[4 * ex + a, 2 * ey + p] for p in range(2)] for a in range(4)]
        fx = [[None] * 2 for _ in range(4)]
        fy = [[None] * 2 for _ in range(4)]
        for a in range(4):
            mix = [u[a][0], swap(u[a][0]), u[a][1], swap(u[a][1])]
            for p in range(2):
                at = (4 * ex + a, 2 * ey + p)
                gx = dot4(D[a], [u[b][p] for b in range(4)])
                gy = dot4(D_half[p], mix)
                m0, mc, m1 = M[(0,) + at], M[(1,) + at], M[(2,) + at]
                fx[a][p] = m0 * gx + mc * gy
                fy[a][p] = mc * gx + m1 * gy
        for a in range(4):
            mix = [fy[a][0], swap(fy[a][0]), fy[a][1], swap(fy[a][1])]
            for p in range(2):
                W[4 * ex + a, 2 * ey + p] = dot4(
                    minus_t[a], [fx[b][p] for b in range(4)]
                ) + dot4(minus_half[p], mix)

    def rows_sum(x, q):
        if x % 4 == 0 and x > 0:
            return W[x, q] + W[x - 1, q]
        if x % 4 == 3 and x < nx - 1:
            return W[x, q] + W[x + 1, q]
        return W[x, q]

    def assemble_row(x):
        line = [rows_sum(x, q) for q in range(nq)]
        for ey in range(1, nby):
            v, w = line[2 * ey - 1], line[2 * ey]
            line[2 * ey - 1], line[2 * ey] = v + high * swap(w), w + low * swap(v)
        for q in range(nq):
            T[x, q] = line[q]
            if x % 4 == 3 and x < nx - 1:
                T[x + 1, q] = line[q]

    def send(phase, k, src, dst):
        copy = pltpu.make_async_remote_copy(
            src_ref=src, dst_ref=dst,
            send_sem=send_sem.at[phase, k], recv_sem=recv_sem.at[phase, opposite[k]],
            device_id=peers[k], device_id_type=MESH,
        )
        copy.start()
        return copy

    def phase_sends(phase, src, sC, rR, rC, rK, ready):
        copies = [None] * 8
        for ex in order[:2]:
            ready(ex)
            for ey in range(nby):
                laplace(src, ex, ey)
        for x in (0, nx - 1):
            assemble_row(x)
        if phase == 0:
            pl.semaphore_wait(barrier, len(peers))
        for s in range(2):
            for t in range(2):
                k = 4 + 2 * s + t
                copies[k] = send(
                    phase, k, W.at[s * (nx - 1), t * (nq - 1)], rK.at[3 - 2 * s - t]
                )
        for s in range(2):
            copies[s] = send(phase, s, T.at[s * (nx - 1)], rR.at[1 - s])
        if phase == 0:
            for k in range(8):
                masses.append(
                    pltpu.make_async_remote_copy(
                        src_ref=mass_ref, dst_ref=rM.at[opposite[k]],
                        send_sem=mass_send.at[k], recv_sem=mass_recv.at[opposite[k]],
                        device_id=peers[k], device_id_type=MESH,
                    )
                )
                masses[-1].start()
        for ex in order[2:]:
            ready(ex)
            for ey in range(nby):
                laplace(src, ex, ey)
        for k in range(nx // 2):
            a, b = rows_sum(2 * k, 0), rows_sum(2 * k + 1, 0)
            sC[0, k] = jnp.where(is_low, a, swap(b))
            a, b = rows_sum(2 * k, nq - 1), rows_sum(2 * k + 1, nq - 1)
            sC[1, k] = jnp.where(is_low, swap(a), b)
        for t in range(2):
            copies[2 + t] = send(phase, 2 + t, sC.at[t], rC.at[1 - t])
        for x in range(1, nx - 1):
            if x % 4 != 0:
                assemble_row(x)
        return copies

    def finished(x, rR, rC, rK):
        line = [T[x, q] for q in range(nq)]
        if x in (0, nx - 1):
            s = 0 if x == 0 else 1
            line = [v + rR[s, q] for q, v in enumerate(line)]
            line[0] = line[0] + low * swap(rK[2 * s])
            line[-1] = line[-1] + high * swap(rK[2 * s + 1])
        before, after = rC[0, x // 2], rC[1, x // 2]
        if x % 2 == 0:
            after = swap(after)
        else:
            before = swap(before)
        line[0] = line[0] + low * before
        line[-1] = line[-1] + high * after
        return line

    masses = []
    first_copies = phase_sends(0, raw, sC1, rR1, rC1, rK1, lambda ex: loads[ex].wait())

    for copy in masses:
        copy.wait_recv()
    x_at = lax.broadcasted_iota(jnp.int32, (nx, ny), 0)
    y_at = lax.broadcasted_iota(jnp.int32, (nx, ny), 1)
    x_low, x_high = (x_at & 3) == 0, (x_at & 3) == 3
    y_low, y_high = (y_at & 3) == 0, (y_at & 3) == 3

    def mass_rows(own, prev, nxt):
        down = jnp.concatenate([prev[nx - 1:], own[: nx - 1]], axis=0)
        up = jnp.concatenate([own[1:], nxt[:1]], axis=0)
        return own + jnp.where(x_low, down, 0.0) + jnp.where(x_high, up, 0.0)

    here = mass_rows(mass_ref[...], rM[0], rM[1])
    left = mass_rows(rM[2], rM[4], rM[6])
    right = mass_rows(rM[3], rM[5], rM[7])
    back = jnp.concatenate([left[:, ny - 1:], here[:, : ny - 1]], axis=1)
    ahead = jnp.concatenate([here[:, 1:], right[:, :1]], axis=1)
    mass_sum = here + jnp.where(y_low, back, 0.0) + jnp.where(y_high, ahead, 0.0)
    split(3, 1.0 / mass_sum)
    for x in range(nx):
        spread_row(3, x)

    for copy in first_copies:
        copy.wait_recv()
    for x in range(nx):
        line = finished(x, rR1, rC1, rK1)
        for q in range(nq):
            U[x, q] = line[q] * M[3, x, q]
    for copy in first_copies:
        copy.wait_send()

    second_copies = phase_sends(1, U, sC2, rR2, rC2, rK2, lambda ex: None)
    for copy in second_copies:
        copy.wait_recv()
    for x in range(nx):
        line = finished(x, rR2, rC2, rK2)
        for q in range(nq):
            out_ref[x, q] = line[q] * M[3, x, q]
    for copy in second_copies + masses:
        copy.wait_send()


def solution(mesh):
    faces, cols = mesh.shape["face"], mesh.shape["col"]

    def shards(fields, metric_diag, metric_cross, point_mass):
        nf, nx, ny, lanes = fields.shape
        nbx, nby = nx // 4, ny // 4
        f32 = jnp.float32
        tiles = (nx, ny // 2, 2 * nf, lanes)

        def vmem(*shape):
            return pltpu.VMEM(shape, f32)

        def landing():
            return [
                vmem(2, nx // 2, 2 * nf, lanes),
                vmem(2, ny // 2, 2 * nf, lanes),
                vmem(2, nx // 2, 2 * nf, lanes),
                vmem(4, 2 * nf, lanes),
            ]

        out = pl.pallas_call(
            functools.partial(kernel, faces, cols, nf, nbx, nby),
            out_shape=jax.ShapeDtypeStruct(tiles, f32),
            in_specs=[pl.BlockSpec(memory_space=pltpu.HBM)] * 4,
            out_specs=pl.BlockSpec(memory_space=pltpu.VMEM),
            scratch_shapes=[
                vmem(nx, 2, ny),
                vmem(nx, ny),
                vmem(nx, ny),
                vmem(*tiles),
                vmem(*tiles),
                vmem(4, *tiles),
                vmem(*tiles),
                vmem(*tiles),
                vmem(4, nx, 3 * ny),
                vmem(8, nx, ny),
                *landing(), *landing(),
                pltpu.SemaphoreType.DMA((3,)),
                pltpu.SemaphoreType.DMA((nbx,)),
                pltpu.SemaphoreType.DMA((8,)),
                pltpu.SemaphoreType.DMA((8,)),
                pltpu.SemaphoreType.DMA((2, 8)),
                pltpu.SemaphoreType.DMA((2, 8)),
            ],
            compiler_params=pltpu.CompilerParams(
                collective_id=0, has_side_effects=True, vmem_limit_bytes=45000000
            ),
        )(
            fields.transpose(1, 2, 0, 3).reshape(tiles),
            metric_diag.transpose(1, 0, 2), metric_cross, point_mass,
        )
        return out.reshape(nx, ny, nf, lanes).transpose(2, 0, 1, 3)

    return jax.shard_map(
        shards,
        mesh=mesh,
        in_specs=(
            P(None, "face", "col", None),
            P(None, "face", "col"),
            P("face", "col"),
            P("face", "col"),
        ),
        out_specs=P(None, "face", "col", None),
        check_vma=False,
    )
```

```python
import functools

import jax
import jax.numpy as jnp
import numpy as np
from jax import lax
from jax.experimental import pallas as pl
from jax.experimental.pallas import tpu as pltpu
from jax.sharding import PartitionSpec as P

MESH = pl.DeviceIdType.MESH


def derivative_table():
    small = 1.0 / np.sqrt(5.0)
    nodes = np.array([-1.0, -small, small, 1.0])
    count = nodes.shape[0]
    weights = np.array(
        [np.prod([nodes[a] - nodes[k] for k in range(count) if k != a]) for a in range(count)]
    )
    table = np.zeros((count, count))
    for a in range(count):
        for b in range(count):
            if a == b:
                table[a, b] = np.sum([1.0 / (nodes[a] - nodes[k]) for k in range(count) if k != a])
            else:
                table[a, b] = weights[a] / weights[b] / (nodes[a] - nodes[b])
    return [[float(np.float32(v)) for v in row] for row in table]


def dot4(coefs, terms):
    total = None
    for c, t in zip(coefs, terms):
        if isinstance(c, float) and c == 0.0:
            continue
        total = c * t if total is None else total + c * t
    return total


def kernel(
    faces, cols, nf, nbx, nby,
    fields_hbm, diag_hbm, cross_hbm, mass_hbm, out_ref,
    diag_ref, cross_ref, mass_ref, raw, U, M, W, T, spread, rM,
    sC1, rR1, rC1, rK1, sC2, rR2, rC2, rK2,
    small_sem, load_sem, mass_send, mass_recv, send_sem, recv_sem,
):
    face, col = lax.axis_index("face"), lax.axis_index("col")
    fside = (lax.rem(face + faces - 1, faces), lax.rem(face + 1, faces))
    cside = (lax.rem(col + cols - 1, cols), lax.rem(col + 1, cols))
    peers = [(fside[0], col), (fside[1], col), (face, cside[0]), (face, cside[1])]
    peers += [(fside[s], cside[t]) for s in range(2) for t in range(2)]
    opposite = [1, 0, 3, 2, 7, 6, 5, 4]

    nx, ny, nq = 4 * nbx, 4 * nby, 2 * nby
    lanes = raw.shape[-1]
    barrier = pltpu.get_barrier_semaphore()
    for peer in peers:
        pl.semaphore_signal(barrier, inc=1, device_id=peer, device_id_type=MESH)

    order = [0, nbx - 1] + list(range(1, nbx - 1))
    loads = {
        ex: pltpu.make_async_copy(
            fields_hbm.at[pl.ds(4 * ex, 4)], raw.at[pl.ds(4 * ex, 4)], load_sem.at[ex]
        )
        for ex in order
    }
    small = [
        pltpu.make_async_copy(src, dst, small_sem.at[k])
        for k, (src, dst) in enumerate(
            ((diag_hbm, diag_ref), (cross_hbm, cross_ref), (mass_hbm, mass_ref))
        )
    ]
    for copy in small:
        copy.start()
    for ex in order:
        loads[ex].start()
    for copy in small:
        copy.wait()

    D = derivative_table()
    sub = lax.broadcasted_iota(jnp.int32, (2 * nf, lanes), 0)
    is_low = sub < nf
    low = jnp.where(is_low, 1.0, 0.0)
    high = 1.0 - low

    def swap(v):
        return pltpu.roll(v, nf, 0)

    def halves(table):
        return [
            [
                jnp.where(is_low, table[2 * p][2 * q + k], table[2 * p + 1][2 * q + 1 - k])
                for q in range(2) for k in range(2)
            ]
            for p in range(2)
        ]

    minus_t = [[-D[b][a] for b in range(4)] for a in range(4)]
    D_half, minus_half = halves(D), halves(minus_t)

    row = lax.broadcasted_iota(jnp.int32, (nf * ny, 3 * ny), 0)
    lane = lax.broadcasted_iota(jnp.int32, (nf * ny, 3 * ny), 1)
    keep = jnp.zeros((nf * ny, 3 * ny), jnp.float32)
    for k in range(3):
        first_row = nf * (lane - k * ny)
        keep = jnp.where((row >= first_row) & (row < first_row + nf), 1.0, keep)
    ones = jnp.ones((3 * ny, lanes), jnp.bfloat16)

    def split(slot, m):
        parts = []
        for _ in range(3):
            part = m.astype(jnp.bfloat16).astype(jnp.float32)
            m = m - part
            parts.append(part)
        spread[slot] = jnp.concatenate(parts, axis=1)

    def spread_row(slot, x):
        left = (keep * spread[slot, pl.ds(x, 1), :]).astype(jnp.bfloat16)
        wide = jnp.dot(left, ones, preferred_element_type=jnp.float32)
        M[slot, x] = wide.reshape(nq, 2 * nf, lanes)

    split(0, diag_ref[:, 0, :])
    split(1, cross_ref[...])
    split(2, diag_ref[:, 1, :])
    for x in range(nx):
        for slot in range(3):
            spread_row(slot, x)

    def laplace(src, ex, ey):
        u = [[src[4 * ex + a, 2 * ey + p] for p in range(2)] for a in range(4)]
        fx = [[None] * 2 for _ in range(4)]
        fy = [[None] * 2 for _ in range(4)]
        for a in range(4):
            mix = [u[a][0], swap(u[a][0]), u[a][1], swap(u[a][1])]
            for p in range(2):
                at = (4 * ex + a, 2 * ey + p)
                gx = dot4(D[a], [u[b][p] for b in range(4)])
                gy = dot4(D_half[p], mix)
                m0, mc, m1 = M[(0,) + at], M[(1,) + at], M[(2,) + at]
                fx[a][p] = m0 * gx + mc * gy
                fy[a][p] = mc * gx + m1 * gy
        for a in range(4):
            mix = [fy[a][0], swap(fy[a][0]), fy[a][1], swap(fy[a][1])]
            for p in range(2):
                W[4 * ex + a, 2 * ey + p] = dot4(
                    minus_t[a], [fx[b][p] for b in range(4)]
                ) + dot4(minus_half[p], mix)

    def rows_sum(x, q):
        if x % 4 == 0 and x > 0:
            return W[x, q] + W[x - 1, q]
        if x % 4 == 3 and x < nx - 1:
            return W[x, q] + W[x + 1, q]
        return W[x, q]

    def assemble_row(x):
        line = [rows_sum(x, q) for q in range(nq)]
        for ey in range(1, nby):
            v, w = line[2 * ey - 1], line[2 * ey]
            line[2 * ey - 1], line[2 * ey] = v + high * swap(w), w + low * swap(v)
        for q in range(nq):
            T[x, q] = line[q]
            if x % 4 == 3 and x < nx - 1:
                T[x + 1, q] = line[q]

    def send(phase, k, src, dst):
        copy = pltpu.make_async_remote_copy(
            src_ref=src, dst_ref=dst,
            send_sem=send_sem.at[phase, k], recv_sem=recv_sem.at[phase, opposite[k]],
            device_id=peers[k], device_id_type=MESH,
        )
        copy.start()
        return copy

    def phase_sends(phase, src, sC, rR, rC, rK, ready):
        copies = [None] * 8
        for ex in order[:2]:
            ready(ex)
            for ey in range(nby):
                laplace(src, ex, ey)
        for x in (0, nx - 1):
            assemble_row(x)
        if phase == 0:
            pl.semaphore_wait(barrier, len(peers))
        for s in range(2):
            for t in range(2):
                k = 4 + 2 * s + t
                copies[k] = send(
                    phase, k, W.at[s * (nx - 1), t * (nq - 1)], rK.at[3 - 2 * s - t]
                )
        for s in range(2):
            copies[s] = send(phase, s, T.at[s * (nx - 1)], rR.at[1 - s])
        if phase == 0:
            for k in range(8):
                masses.append(
                    pltpu.make_async_remote_copy(
                        src_ref=mass_ref, dst_ref=rM.at[opposite[k]],
                        send_sem=mass_send.at[k], recv_sem=mass_recv.at[opposite[k]],
                        device_id=peers[k], device_id_type=MESH,
                    )
                )
                masses[-1].start()
        for ex in order[2:]:
            ready(ex)
            for ey in range(nby):
                laplace(src, ex, ey)
        for k in range(nx // 2):
            a, b = rows_sum(2 * k, 0), rows_sum(2 * k + 1, 0)
            sC[0, k] = jnp.where(is_low, a, swap(b))
            a, b = rows_sum(2 * k, nq - 1), rows_sum(2 * k + 1, nq - 1)
            sC[1, k] = jnp.where(is_low, swap(a), b)
        for t in range(2):
            copies[2 + t] = send(phase, 2 + t, sC.at[t], rC.at[1 - t])
        for x in range(1, nx - 1):
            if x % 4 != 0:
                assemble_row(x)
        return copies

    def finished(x, rR, rC, rK):
        line = [T[x, q] for q in range(nq)]
        if x in (0, nx - 1):
            s = 0 if x == 0 else 1
            line = [v + rR[s, q] for q, v in enumerate(line)]
            line[0] = line[0] + low * swap(rK[2 * s])
            line[-1] = line[-1] + high * swap(rK[2 * s + 1])
        before, after = rC[0, x // 2], rC[1, x // 2]
        if x % 2 == 0:
            after = swap(after)
        else:
            before = swap(before)
        line[0] = line[0] + low * before
        line[-1] = line[-1] + high * after
        return line

    masses = []
    first_copies = phase_sends(0, raw, sC1, rR1, rC1, rK1, lambda ex: loads[ex].wait())

    for copy in masses:
        copy.wait_recv()
    x_at = lax.broadcasted_iota(jnp.int32, (nx, ny), 0)
    y_at = lax.broadcasted_iota(jnp.int32, (nx, ny), 1)
    x_low, x_high = (x_at & 3) == 0, (x_at & 3) == 3
    y_low, y_high = (y_at & 3) == 0, (y_at & 3) == 3

    def mass_rows(own, prev, nxt):
        down = jnp.concatenate([prev[nx - 1:], own[: nx - 1]], axis=0)
        up = jnp.concatenate([own[1:], nxt[:1]], axis=0)
        return own + jnp.where(x_low, down, 0.0) + jnp.where(x_high, up, 0.0)

    here = mass_rows(mass_ref[...], rM[0], rM[1])
    left = mass_rows(rM[2], rM[4], rM[6])
    right = mass_rows(rM[3], rM[5], rM[7])
    back = jnp.concatenate([left[:, ny - 1:], here[:, : ny - 1]], axis=1)
    ahead = jnp.concatenate([here[:, 1:], right[:, :1]], axis=1)
    mass_sum = here + jnp.where(y_low, back, 0.0) + jnp.where(y_high, ahead, 0.0)
    split(3, 1.0 / mass_sum)
    for x in range(nx):
        spread_row(3, x)

    for copy in first_copies:
        copy.wait_recv()
    for x in range(nx):
        line = finished(x, rR1, rC1, rK1)
        for q in range(nq):
            U[x, q] = line[q] * M[3, x, q]
    for copy in first_copies:
        copy.wait_send()

    second_copies = phase_sends(1, U, sC2, rR2, rC2, rK2, lambda ex: None)
    for copy in second_copies:
        copy.wait_recv()
    for x in range(nx):
        line = finished(x, rR2, rC2, rK2)
        for q in range(nq):
            out_ref[x, q] = line[q] * M[3, x, q]
    for copy in second_copies + masses:
        copy.wait_send()


def solution(mesh):
    faces, cols = mesh.shape["face"], mesh.shape["col"]

    def shards(fields, metric_diag, metric_cross, point_mass):
        nf, nx, ny, lanes = fields.shape
        nbx, nby = nx // 4, ny // 4
        f32 = jnp.float32
        tiles = (nx, ny // 2, 2 * nf, lanes)

        def vmem(*shape):
            return pltpu.VMEM(shape, f32)

        def landing():
            return [
                vmem(2, nx // 2, 2 * nf, lanes),
                vmem(2, ny // 2, 2 * nf, lanes),
                vmem(2, nx // 2, 2 * nf, lanes),
                vmem(4, 2 * nf, lanes),
            ]

        out = pl.pallas_call(
            functools.partial(kernel, faces, cols, nf, nbx, nby),
            out_shape=jax.ShapeDtypeStruct(tiles, f32),
            in_specs=[pl.BlockSpec(memory_space=pltpu.HBM)] * 4,
            out_specs=pl.BlockSpec(memory_space=pltpu.VMEM),
            scratch_shapes=[
                vmem(nx, 2, ny),
                vmem(nx, ny),
                vmem(nx, ny),
                vmem(*tiles),
                vmem(*tiles),
                vmem(4, *tiles),
                vmem(*tiles),
                vmem(*tiles),
                vmem(4, nx, 3 * ny),
                vmem(8, nx, ny),
                *landing(), *landing(),
                pltpu.SemaphoreType.DMA((3,)),
                pltpu.SemaphoreType.DMA((nbx,)),
                pltpu.SemaphoreType.DMA((8,)),
                pltpu.SemaphoreType.DMA((8,)),
                pltpu.SemaphoreType.DMA((2, 8)),
                pltpu.SemaphoreType.DMA((2, 8)),
            ],
            compiler_params=pltpu.CompilerParams(
                collective_id=0, has_side_effects=True, vmem_limit_bytes=32 * 1024 * 1024
            ),
        )(*[
            pltpu.with_memory_space_constraint(v, pltpu.HBM)
            for v in (
                fields.transpose(1, 2, 0, 3).reshape(tiles),
                metric_diag.transpose(1, 0, 2), metric_cross, point_mass,
            )
        ])
        return out.reshape(nx, ny, nf, lanes).transpose(2, 0, 1, 3)

    return jax.shard_map(
        shards,
        mesh=mesh,
        in_specs=(
            P(None, "face", "col", None),
            P(None, "face", "col"),
            P("face", "col"),
            P("face", "col"),
        ),
        out_specs=P(None, "face", "col", None),
        check_vma=False,
    )
```

```python
import functools

import jax
import jax.numpy as jnp
import numpy as np
from jax import lax
from jax.experimental import pallas as pl
from jax.experimental.pallas import tpu as pltpu
from jax.sharding import PartitionSpec as P

MESH = pl.DeviceIdType.MESH


def derivative_table():
    small = 1.0 / np.sqrt(5.0)
    nodes = np.array([-1.0, -small, small, 1.0])
    count = nodes.shape[0]
    weights = np.array(
        [np.prod([nodes[a] - nodes[k] for k in range(count) if k != a]) for a in range(count)]
    )
    table = np.zeros((count, count))
    for a in range(count):
        for b in range(count):
            if a == b:
                table[a, b] = np.sum([1.0 / (nodes[a] - nodes[k]) for k in range(count) if k != a])
            else:
                table[a, b] = weights[a] / weights[b] / (nodes[a] - nodes[b])
    return [[float(np.float32(v)) for v in row] for row in table]


def add(a, b):
    if a is None or b is None:
        return b if a is None else a
    return a + b


def mul(a, b):
    return None if b is None else a * b


def combine(coefs, terms):
    total = None
    for c, t in zip(coefs, terms):
        if isinstance(c, float) and c == 0.0:
            continue
        total = add(total, mul(c, t))
    return total


def kernel(
    faces, cols, nf, nbx, nby,
    fields_hbm, diag_hbm, cross_hbm, mass_hbm, out_ref,
    diag_ref, cross_ref, mass_ref, raw, U, W, T, side, met, B, Br, Bc, Bd,
    sRA, sRB, sCA, sCB, sD, rRA, rRB, rCA, rCB, rD, rMr, rMc, rMd,
    small_sem, load_sem, send_sem, recv_sem, late,
):
    face, col = lax.axis_index("face"), lax.axis_index("col")
    fside = (lax.rem(face + faces - 1, faces), lax.rem(face + 1, faces))
    cside = (lax.rem(col + cols - 1, cols), lax.rem(col + 1, cols))
    peers = [(fside[0], col), (fside[1], col), (face, cside[0]), (face, cside[1])]
    peers += [(fside[s], cside[t]) for s in range(2) for t in range(2)]
    opposite = [1, 0, 3, 2, 7, 6, 5, 4]
    before, after = [0, 4, 5], [1, 6, 7]

    barrier = pltpu.get_barrier_semaphore()
    for k in (2, 3, *before):
        pl.semaphore_signal(barrier, inc=1, device_id=peers[k], device_id_type=MESH)

    @pl.when(face != faces - 1)
    def _():
        for k in after:
            pl.semaphore_signal(barrier, inc=1, device_id=peers[k], device_id_type=MESH)

    nx, ny, nq = 4 * nbx, 4 * nby, 2 * nby
    lanes = raw.shape[-1]
    tile = (2 * nf, lanes)
    order = [nbx - 1, nbx - 2] + list(range(nbx - 2))
    small = [
        pltpu.make_async_copy(src, dst, small_sem.at[k])
        for k, (src, dst) in enumerate(
            ((diag_hbm, diag_ref), (cross_hbm, cross_ref), (mass_hbm, mass_ref))
        )
    ]
    loads = {
        ex: pltpu.make_async_copy(
            fields_hbm.at[pl.ds(4 * ex, 4)], raw.at[pl.ds(4 * ex, 4)], load_sem.at[ex]
        )
        for ex in order
    }
    for copy in small:
        copy.start()
    for ex in order:
        loads[ex].start()

    D = derivative_table()
    is_low = lax.broadcasted_iota(jnp.int32, tile, 0) < nf
    lane = lax.broadcasted_iota(jnp.int32, tile, 1)
    low = jnp.where(is_low, 1.0, 0.0)
    high = 1.0 - low

    def swap(v):
        return pltpu.roll(v, nf, 0)

    def halves(table):
        return [
            [
                jnp.where(is_low, table[2 * p][2 * q + k], table[2 * p + 1][2 * q + 1 - k])
                for q in range(2) for k in range(2)
            ]
            for p in range(2)
        ]

    minus_t = [[-D[b][a] for b in range(4)] for a in range(4)]
    D_half, minus_half = halves(D), halves(minus_t)

    def mixed(v, w):
        return [v, None if v is None else swap(v), w, None if w is None else swap(w)]

    def laplace(u, m):
        @functools.cache
        def mix(a):
            return mixed(*u[a])

        @functools.cache
        def flux(a, p):
            gx = combine(D[a], [u[b][p] for b in range(4)])
            gy = combine(D_half[p], mix(a))
            return gx, gy

        @functools.cache
        def fx(a, p):
            gx, gy = flux(a, p)
            return add(
                None if gx is None else m(0, a, p) * gx, None if gy is None else m(1, a, p) * gy
            )

        @functools.cache
        def mix_fy(a):
            parts = []
            for p in range(2):
                gx, gy = flux(a, p)
                parts.append(add(
                    None if gx is None else m(1, a, p) * gx, None if gy is None else m(2, a, p) * gy
                ))
            return mixed(*parts)

        def w(a, p):
            return add(
                combine(minus_t[a], [fx(b, p) for b in range(4)]), combine(minus_half[p], mix_fy(a))
            )

        return w

    def wide(row):
        return jnp.broadcast_to(row, tile)

    def in_all_lanes(v, y):
        return jnp.broadcast_to(v[:, y:y + 1], tile)

    def tile_of(column, p):
        return jnp.where(is_low, wide(column(2 * p)), wide(column(2 * p + 1)))

    def metrics(ref, *at):
        return functools.cache(
            lambda slot, a, p: tile_of(lambda j: ref[(*at, j, pl.ds(4 * slot + a, 1))], p)
        )

    def own_metrics(ex, ey):
        return functools.cache(lambda slot, a, p: tile_of(
            lambda j: B[ex, 4 * ey + j, 4 * slot + a:4 * slot + a + 1, :], p
        ))

    def inverse_mass(x, q):
        return own_metrics(x // 4, q // 2)(3, x % 4, q % 2)

    def send(phase, k, src, dst, start=True):
        copy = pltpu.make_async_remote_copy(
            src_ref=src, dst_ref=dst,
            send_sem=send_sem.at[phase, k], recv_sem=recv_sem.at[phase, opposite[k]],
            device_id=peers[k], device_id_type=MESH,
        )
        if start:
            copy.start()
        copies[phase, k] = copy
        return copy

    def arrived(phase, k):
        copies[phase, opposite[k]].wait_recv()

    held = []

    def send_back(*those):
        made = [send(*one, start=False) for one in those]
        held.extend(made)

        @pl.when(face != 0)
        def _():
            for copy in made:
                copy.start()

    copies = {}

    for copy in small:
        copy.wait()
    mass = mass_ref[...]
    x_at = lax.broadcasted_iota(jnp.int32, (nx, ny), 0)
    y_at = lax.broadcasted_iota(jnp.int32, (nx, ny), 1)
    zero_row, zero_col = jnp.zeros((1, ny), jnp.float32), jnp.zeros((nx, 1), jnp.float32)
    down = jnp.concatenate([zero_row, mass[: nx - 1]], axis=0)
    up = jnp.concatenate([mass[1:], zero_row], axis=0)
    mass = mass + jnp.where((x_at & 3) == 0, down, 0.0) + jnp.where((x_at & 3) == 3, up, 0.0)
    back = jnp.concatenate([zero_col, mass[:, : ny - 1]], axis=1)
    ahead = jnp.concatenate([mass[:, 1:], zero_col], axis=1)
    mass = mass + jnp.where((y_at & 3) == 0, back, 0.0) + jnp.where((y_at & 3) == 3, ahead, 0.0)
    cross = cross_ref[...]
    for slot, v in enumerate((diag_ref[:, 0, :], cross, diag_ref[:, 1, :], mass)):
        for ex in range(nbx):
            met[ex, 4 * slot:4 * slot + 4, :ny] = v[4 * ex:4 * ex + 4]

    pl.semaphore_wait(barrier, jnp.where(face == 0, 5, 8))

    @pl.when(face == faces - 1)
    def _():
        for k in after:
            pl.semaphore_signal(late, inc=1, device_id=peers[k], device_id_type=MESH)

    send(0, 1, met.at[nbx - 1], rMr.at[0])
    for t in range(2):
        send(0, 6 + t, met.at[nbx - 1], rMd.at[1 - t])
    for t in range(2):
        send(0, 2 + t, met, rMc.at[1 - t])
    send_back((0, 0, met.at[0], rMr.at[1]), (0, 4, met.at[0], rMd.at[3]), (0, 5, met.at[0], rMd.at[2]))

    sub = lax.broadcasted_iota(jnp.int32, tile, 0)
    halves_of = [pl.ds(8 * i, 8) for i in range(2)]

    def inverted(ex, mass_of=lambda v: v):
        v = met[ex, halves_of[1], :]
        return jnp.where(sub < 4, v, 1.0 / mass_of(v))

    for ex in order:
        v, w = met[ex, halves_of[0], :], inverted(ex)
        for y in range(ny):
            B[ex, y, halves_of[0], :] = in_all_lanes(v, y)
            B[ex, y, halves_of[1], :] = in_all_lanes(w, y)

    def lift(ref, at, to, ys):
        for half in halves_of:
            v = ref[(*at, half)]
            for i, y in enumerate(ys):
                to[(*at, i, half)] = in_all_lanes(v, y)

    def rows_sum(src, x, *at):
        if x % 4 == 0 and x > 0:
            return src(x, *at) + src(x - 1, *at)
        if x % 4 == 3 and x < nx - 1:
            return src(x, *at) + src(x + 1, *at)
        return src(x, *at)

    def across(line):
        for ey in range(1, nby):
            v, w = line[2 * ey - 1], line[2 * ey]
            line[2 * ey - 1], line[2 * ey] = v + high * swap(w), w + low * swap(v)
        return line

    def in_W(x, q):
        return W[x, q]

    def first_laplacian(ex):
        loads[ex].wait()
        for ey in range(nby):
            w = laplace(
                [[raw[4 * ex + a, 2 * ey + p] for p in range(2)] for a in range(4)],
                own_metrics(ex, ey),
            )
            for a in range(4):
                for p in range(2):
                    W[4 * ex + a, 2 * ey + p] = w(a, p)

    def first_rows(xs):
        for x in xs:
            if x % 4 == 0 and x > 0:
                continue
            line = across([rows_sum(in_W, x, q) for q in range(nq)])
            for q in range(nq):
                T[x, q] = line[q]
                if x % 4 == 3 and x < nx - 1:
                    T[x + 1, q] = line[q]

    def inner_first(xs):
        for x in xs:
            for q in range(nq):
                v = T[x, q] * inverse_mass(x, q)
                U[x, q] = high * v if q == 0 else low * v if q == nq - 1 else v

    def known(ex, ey):
        return [
            [None if x in (0, nx - 1) else U[x, 2 * ey + p] for p in range(2)]
            for x in range(4 * ex, 4 * ex + 4)
        ]

    def known_parts(ex):
        edge = {0: (0, 0), nbx - 1: (1, 3)}.get(ex)
        line = [None] * nq
        for ey in range(nby):
            if edge is None and 0 < ey < nby - 1:
                continue
            w = laplace(known(ex, ey), own_metrics(ex, ey))
            if edge:
                line[2 * ey], line[2 * ey + 1] = w(edge[1], 0), w(edge[1], 1)
            for t, e in ((0, 0), (1, nby - 1)):
                if ey == e:
                    for a in range(4):
                        side[t, 4 * ex + a] = w(a, t)
        if edge:
            line = across(line)
            for q in range(nq):
                sRB[edge[0], q] = line[q]

    def stage_row(s):
        xe, near = s * (nx - 1), (nx - 4 if s else 1)
        for q in range(nq):
            sRA[s, q] = T[xe, q]
        for i in range(3):
            sRA[s, nq + i] = jnp.where(is_low, T[near + i, 0], T[near + i, nq - 1])

    def stage_corner(s, t):
        xe, near, q = s * (nx - 1), (nx - 4 if s else 1), t * (nq - 1)
        for p in range(2):
            sD[2 * s + t, p] = T[xe, t * (nq - 2) + p]
        halves = [T[near + i, q] for i in range(3)] + [sRB[s, q]]
        for i in range(2):
            v, w = halves[2 * i], halves[2 * i + 1]
            sD[2 * s + t, 2 + i] = (
                jnp.where(is_low, swap(v), w) if t else jnp.where(is_low, v, swap(w))
            )

    def pack_column(t, v, w):
        return jnp.where(is_low, swap(v), w) if t else jnp.where(is_low, v, swap(w))

    for ex in order[:2]:
        first_laplacian(ex)
    first_rows(range(nx - 5, nx))
    stage_row(1)
    send(1, 1, sRA.at[1], rRA.at[0])
    inner_first(range(nx - 4, nx - 1))
    known_parts(nbx - 1)
    for t in range(2):
        stage_corner(1, t)
        send(1, 6 + t, sD.at[2 + t], rD.at[1 - t])
    send(2, 1, sRB.at[1], rRB.at[0])

    for ex in order[2:]:
        first_laplacian(ex)
    first_rows(range(nx - 5))
    for t in range(2):
        q = t * (nq - 1)
        for k in range(nx // 2):
            sCA[t, k] = pack_column(t, T[2 * k, q], T[2 * k + 1, q])
        for s in range(2):
            for p in range(2):
                sCA[t, nx // 2 + 2 * s + p] = T[s * (nx - 1), t * (nq - 2) + p]
        send(1, 2 + t, sCA.at[t], rCA.at[1 - t])
    stage_row(0)
    send_back((1, 0, sRA.at[0], rRA.at[1]))
    inner_first(range(1, nx - 4))
    for ex in range(nbx - 1):
        known_parts(ex)
    for t in range(2):
        stage_corner(0, t)
    send_back(
        (1, 4, sD.at[0], rD.at[3]), (1, 5, sD.at[1], rD.at[2]), (2, 0, sRB.at[0], rRB.at[1])
    )
    for t in range(2):
        def in_side(x, t=t):
            return side[t, x]

        for k in range(nx // 2):
            sCB[t, k] = pack_column(t, rows_sum(in_side, 2 * k), rows_sum(in_side, 2 * k + 1))
        send(2, 2 + t, sCB.at[t], rCB.at[1 - t])

    @pl.when(face == 0)
    def _():
        pl.semaphore_wait(late, 3)
        for copy in held:
            copy.start()

    def mass_row(ref, *at):
        return wide(ref[(*at[:-1], pl.ds(12 + at[-1], 1))])

    def with_sides(mid, left, right):
        return (
            mid
            + jnp.where(lane == 0, pltpu.roll(left, lanes - (ny - 1), 1), 0.0)
            + jnp.where(lane == ny - 1, pltpu.roll(right, ny - 1, 1), 0.0)
        )

    def column_part(ref, t, x):
        v = ref[t, x // 2]
        if x % 2 != t:
            v = swap(v)
        return (high if t else low) * v

    def second_elements(ex, eys):
        for ey in eys:
            w = laplace(
                [[U[4 * ex + a, 2 * ey + p] for p in range(2)] for a in range(4)],
                own_metrics(ex, ey),
            )
            for a in range(4):
                for p in range(2):
                    W[4 * ex + a, 2 * ey + p] = w(a, p)

    def side_elements(t, ex, row=None, ext=None):
        u = []
        for a in range(4):
            v = swap(U[4 * ex + a, t * (nq - 1)])
            u.append([low * v, None] if t else [None, high * v])
        if row is not None:
            u[row] = ext
        w = laplace(u, metrics(Bc, t, ex))
        for a in range(4):
            side[t, 4 * ex + a] = w(a, 1 - t)

    inner = range(1, nby - 1)
    for ex in range(1, nbx - 1):
        second_elements(ex, inner)
    for t in range(2):
        arrived(0, 2 + t)
    for ex in range(nbx):
        v = inverted(ex, lambda v: with_sides(
            v, rMc[0, ex, halves_of[1], :], rMc[1, ex, halves_of[1], :]
        ))
        for y in (0, ny - 1):
            B[ex, y, halves_of[1], :] = in_all_lanes(v, y)
        for t in range(2):
            lift(rMc, (t, ex), Bc, range(4) if t else range(ny - 4, ny))
    for t in range(2):
        arrived(1, 2 + t)
    for x in range(1, nx - 1):
        for t in range(2):
            q = t * (nq - 1)
            U[x, q] = (T[x, q] + column_part(rCA, t, x)) * inverse_mass(x, q)
    for ex in range(1, nbx - 1):
        second_elements(ex, (0, nby - 1))
        for t in range(2):
            side_elements(t, ex)
    for t in range(2):
        arrived(2, 2 + t)

    def finish(x, halo=None, corner=None):
        line = [rows_sum(in_W, x, q) for q in range(nq)]
        if halo:
            line = [add(v, h) for v, h in zip(line, halo)]
        line = across(line)
        s = 0 if x == 0 else 1
        if halo:
            line = [v + rRB[s, q] for q, v in enumerate(line)]
        for t in range(2):
            q = t * (nq - 1)
            v = rows_sum(lambda x: side[t, x], x)
            if corner:
                v = v + corner[t]
            v = swap(v)
            if corner:
                last = rD[2 * s + t, 3]
                v = v + (last if t else swap(last))
            line[q] = line[q] + (high if t else low) * v + column_part(rCB, t, x)
        for at in [x] + ([x + 1] if x % 4 == 3 and x < nx - 1 else []):
            for q in range(nq):
                out_ref[at, q] = line[q] * inverse_mass(at, q)

    for x in range(5, nx - 5):
        if x % 4:
            finish(x)

    def ring_rows(s):
        xe, ex, own_row, halo_row = s * (nx - 1), s * (nbx - 1), 3 * s, 3 - 3 * s
        rest = [a for a in range(4) if a != halo_row]
        arrived(0, s)
        for t in range(2):
            arrived(0, 4 + 2 * s + t)

        own = sub == 4 + own_row
        v = inverted(ex, lambda v: with_sides(
            v + jnp.where(own, mass_row(rMr, s, halo_row), 0.0),
            *[
                rMc[t, ex, halves_of[1], :] + jnp.where(own, mass_row(rMd, 2 * s + t, halo_row), 0.0)
                for t in range(2)
            ],
        ))
        for y in range(ny):
            B[ex, y, halves_of[1], :] = in_all_lanes(v, y)
        lift(rMr, (s,), Br, range(ny))
        for t in range(2):
            lift(rMd, (2 * s + t,), Bd, range(4) if t else range(ny - 4, ny))
        inv_ext = []
        for t in range(2):
            v = 1.0 / (mass_row(rMc, t, ex, own_row) + mass_row(rMd, 2 * s + t, halo_row))
            y = (1 - t) * (ny - 4)
            inv_ext.append([
                jnp.where(is_low, in_all_lanes(v, y + 2 * p), in_all_lanes(v, y + 2 * p + 1))
                for p in range(2)
            ])
        inv_beyond = []
        for a in rest:
            v = 1.0 / with_sides(
                mass_row(rMr, s, a), mass_row(rMd, 2 * s, a), mass_row(rMd, 2 * s + 1, a)
            )
            inv_beyond.append(jnp.where(is_low, in_all_lanes(v, 0), in_all_lanes(v, ny - 1)))

        arrived(1, s)
        for t in range(2):
            arrived(1, 4 + 2 * s + t)
        for q in range(nq):
            v = T[xe, q] + rRA[s, q]
            for t in range(2):
                if q == t * (nq - 1):
                    v = v + column_part(rCA, t, xe)
                    v = v + (high if t else low) * swap(rD[2 * s + t, 1 - t])
            U[xe, q] = v * inverse_mass(xe, q)
        ext = []
        for t in range(2):
            e = [
                (rCA[t, nx // 2 + 2 * s + p] + rD[2 * s + t, p]) * inv_ext[t][p] for p in range(2)
            ]
            corner = swap(U[xe, t * (nq - 1)])
            e[1 - t] = high * e[0] + low * corner if t else low * e[1] + high * corner
            ext.append(e)
        beyond = []
        for i in range(3):
            v, w = rD[2 * s, 2 + i // 2], rD[2 * s + 1, 2 + i // 2]
            v, w = (swap(v), w) if i % 2 else (v, swap(w))
            beyond.append((rRA[s, nq + i] + low * v + high * w) * inv_beyond[i])

        second_elements(ex, range(nby))
        for t in range(2):
            side_elements(t, ex, own_row, ext[t])
        halo = []
        for ey in range(nby):
            u = [[None, None] for _ in range(4)]
            u[halo_row] = [U[xe, 2 * ey + p] for p in range(2)]
            for i, a in enumerate(rest):
                if ey == 0:
                    u[a][0] = low * beyond[i]
                if ey == nby - 1:
                    u[a][1] = high * beyond[i]
            w = laplace(u, functools.cache(lambda slot, a, p, ey=ey: tile_of(
                lambda j: Br[s, 4 * ey + j, 4 * slot + a:4 * slot + a + 1, :], p
            )))
            halo += [w(halo_row, 0), w(halo_row, 1)]
        corner = []
        for t in range(2):
            u = [[None, None] for _ in range(4)]
            u[halo_row] = ext[t]
            for i, a in enumerate(rest):
                v = swap(beyond[i])
                u[a] = [low * v, None] if t else [None, high * v]
            w = laplace(u, metrics(Bd, 2 * s + t))
            corner.append(w(halo_row, 1 - t))
        for x in (range(nx - 5, nx) if s else range(5)):
            if x % 4 and x != xe:
                finish(x)
        arrived(2, s)
        finish(xe, halo, corner)

    ring_rows(1)
    ring_rows(0)
    for copy in copies.values():
        copy.wait_send()


def solution(mesh):
    faces, cols = mesh.shape["face"], mesh.shape["col"]

    def shards(fields, metric_diag, metric_cross, point_mass):
        nf, nx, ny, lanes = fields.shape
        nbx, nby = nx // 4, ny // 4
        nq = ny // 2
        f32 = jnp.float32
        tiles = (nx, nq, 2 * nf, lanes)

        def vmem(*shape):
            return pltpu.VMEM(shape, f32)

        def messages():
            return [
                vmem(2, nq + 3, 2 * nf, lanes),
                vmem(2, nq, 2 * nf, lanes),
                vmem(2, nx // 2 + 4, 2 * nf, lanes),
                vmem(2, nx // 2, 2 * nf, lanes),
                vmem(4, 4, 2 * nf, lanes),
            ]

        out = pl.pallas_call(
            functools.partial(kernel, faces, cols, nf, nbx, nby),
            out_shape=jax.ShapeDtypeStruct(tiles, f32),
            in_specs=[pl.BlockSpec(memory_space=pltpu.HBM)] * 4,
            out_specs=pl.BlockSpec(memory_space=pltpu.VMEM),
            scratch_shapes=[
                vmem(nx, 2, ny),
                vmem(nx, ny),
                vmem(nx, ny),
                vmem(*tiles),
                vmem(*tiles),
                vmem(*tiles),
                vmem(*tiles),
                vmem(2, nx, 2 * nf, lanes),
                vmem(nbx, 16, lanes),
                vmem(nbx, ny, 16, lanes),
                vmem(2, ny, 16, lanes),
                vmem(2, nbx, 4, 16, lanes),
                vmem(4, 4, 16, lanes),
                *messages(), *messages(),
                vmem(2, 16, lanes),
                vmem(2, nbx, 16, lanes),
                vmem(4, 16, lanes),
                pltpu.SemaphoreType.DMA((3,)),
                pltpu.SemaphoreType.DMA((nbx,)),
                pltpu.SemaphoreType.DMA((3, 8)),
                pltpu.SemaphoreType.DMA((3, 8)),
                pltpu.SemaphoreType.REGULAR,
            ],
            compiler_params=pltpu.CompilerParams(
                collective_id=0, has_side_effects=True, vmem_limit_bytes=32 * 1024 * 1024
            ),
        )(*[
            pltpu.with_memory_space_constraint(v, pltpu.HBM)
            for v in (
                fields.transpose(1, 2, 0, 3).reshape(tiles),
                metric_diag.transpose(1, 0, 2), metric_cross, point_mass,
            )
        ])
        return out.reshape(nx, ny, nf, lanes).transpose(2, 0, 1, 3)

    return jax.shard_map(
        shards,
        mesh=mesh,
        in_specs=(
            P(None, "face", "col", None),
            P(None, "face", "col"),
            P("face", "col"),
            P("face", "col"),
        ),
        out_specs=P(None, "face", "col", None),
        check_vma=False,
    )
```

```python
import functools

import jax
import jax.numpy as jnp
import numpy as np
from jax import lax
from jax.experimental import pallas as pl
from jax.experimental.pallas import tpu as pltpu
from jax.sharding import PartitionSpec as P

MESH = pl.DeviceIdType.MESH


def derivative_table():
    small = 1.0 / np.sqrt(5.0)
    nodes = np.array([-1.0, -small, small, 1.0])
    count = nodes.shape[0]
    weights = np.array(
        [np.prod([nodes[a] - nodes[k] for k in range(count) if k != a]) for a in range(count)]
    )
    table = np.zeros((count, count))
    for a in range(count):
        for b in range(count):
            if a == b:
                table[a, b] = np.sum([1.0 / (nodes[a] - nodes[k]) for k in range(count) if k != a])
            else:
                table[a, b] = weights[a] / weights[b] / (nodes[a] - nodes[b])
    return [[float(np.float32(v)) for v in row] for row in table]


def add(a, b):
    if a is None or b is None:
        return b if a is None else a
    return a + b


def mul(a, b):
    return None if b is None else a * b


def combine(coefs, terms):
    total = None
    for c, t in zip(coefs, terms):
        if isinstance(c, float) and c == 0.0:
            continue
        total = add(total, mul(c, t))
    return total


def kernel(
    faces, cols, nf, nbx, nby,
    fields_hbm, diag_hbm, cross_hbm, mass_hbm, out_ref,
    diag_ref, cross_ref, mass_ref, raw, U, W, T, side, met, B, Br, Bc, Bd, inv,
    sM, sA, sRB, sCA, sCB, rMc, rMr, rA, rRB, rCA, rCB, sent,
    small_sem, load_sem, send_sem, recv_sem, late,
):
    face, col = lax.axis_index("face"), lax.axis_index("col")
    fside = (lax.rem(face + faces - 1, faces), lax.rem(face + 1, faces))
    cside = (lax.rem(col + cols - 1, cols), lax.rem(col + 1, cols))
    peers = [(fside[0], col), (fside[1], col), (face, cside[0]), (face, cside[1])]
    peers += [(fside[s], cside[t]) for s in range(2) for t in range(2)]
    opposite = [1, 0, 3, 2, 7, 6, 5, 4]
    before, after = [0, 4, 5], [1, 6, 7]

    barrier = pltpu.get_barrier_semaphore()
    for k in (2, 3, *before):
        pl.semaphore_signal(barrier, inc=1, device_id=peers[k], device_id_type=MESH)

    @pl.when(face != faces - 1)
    def _():
        for k in after:
            pl.semaphore_signal(barrier, inc=1, device_id=peers[k], device_id_type=MESH)

    nx, ny, nq = 4 * nbx, 4 * nby, 2 * nby
    lanes = raw.shape[-1]
    tile = (2 * nf, lanes)
    corner_at = [nq + 3, nq + 7]
    small = [
        pltpu.make_async_copy(src, dst, small_sem.at[k])
        for k, (src, dst) in enumerate(
            ((diag_hbm, diag_ref), (cross_hbm, cross_ref), (mass_hbm, mass_ref))
        )
    ]
    load = pltpu.make_async_copy(fields_hbm, raw, load_sem)
    for copy in small:
        copy.start()
    load.start()

    D = derivative_table()
    is_low = lax.broadcasted_iota(jnp.int32, tile, 0) < nf
    lane = lax.broadcasted_iota(jnp.int32, tile, 1)
    low = jnp.where(is_low, 1.0, 0.0)
    high = 1.0 - low

    def swap(v):
        return pltpu.roll(v, nf, 0)

    def halves(table):
        return [
            [
                jnp.where(is_low, table[2 * p][2 * q + k], table[2 * p + 1][2 * q + 1 - k])
                for q in range(2) for k in range(2)
            ]
            for p in range(2)
        ]

    minus_t = [[-D[b][a] for b in range(4)] for a in range(4)]
    D_half, minus_half = halves(D), halves(minus_t)

    def mixed(v, w):
        return [v, None if v is None else swap(v), w, None if w is None else swap(w)]

    def laplace(u, m):
        @functools.cache
        def mix(a):
            return mixed(*u[a])

        @functools.cache
        def flux(a, p):
            gx = combine(D[a], [u[b][p] for b in range(4)])
            gy = combine(D_half[p], mix(a))
            return gx, gy

        @functools.cache
        def fx(a, p):
            gx, gy = flux(a, p)
            return add(
                None if gx is None else m(0, a, p) * gx, None if gy is None else m(1, a, p) * gy
            )

        @functools.cache
        def mix_fy(a):
            parts = []
            for p in range(2):
                gx, gy = flux(a, p)
                parts.append(add(
                    None if gx is None else m(1, a, p) * gx, None if gy is None else m(2, a, p) * gy
                ))
            return mixed(*parts)

        def w(a, p):
            return add(
                combine(minus_t[a], [fx(b, p) for b in range(4)]), combine(minus_half[p], mix_fy(a))
            )

        return w

    def wide(row):
        return jnp.broadcast_to(row, tile)

    def in_all_lanes(v, y):
        return jnp.broadcast_to(v[:, y:y + 1], tile)

    def tile_of(column, p):
        return jnp.where(is_low, wide(column(2 * p)), wide(column(2 * p + 1)))

    def metrics(ref, *at):
        return functools.cache(
            lambda slot, a, p: tile_of(lambda j: ref[(*at, j, pl.ds(4 * slot + a, 1))], p)
        )

    def own_metrics(ex, ey):
        return functools.cache(lambda slot, a, p: tile_of(
            lambda j: B[ex, 4 * ey + j, 4 * slot + a:4 * slot + a + 1, :], p
        ))

    def inverse_mass(x, q):
        return own_metrics(x // 4, q // 2)(3, x % 4, q % 2)

    def copy_of(group, k, src, dst):
        return pltpu.make_async_remote_copy(
            src_ref=src, dst_ref=dst, send_sem=send_sem, recv_sem=recv_sem.at[group],
            device_id=peers[k], device_id_type=MESH,
        )

    def arrived(group, landed):
        pltpu.make_async_remote_copy(
            src_ref=landed, dst_ref=landed, send_sem=send_sem, recv_sem=recv_sem.at[group],
            device_id=peers[0], device_id_type=MESH,
        ).wait_recv()

    def row_metrics(s):
        return [copy_of(3 + 3 * (1 - s), s, sM.at[s], rMr.at[1 - s, 0])] + [
            copy_of(3 + 3 * (1 - s), 4 + 2 * s + t, sM.at[s], rMr.at[1 - s, 2 - t]) for t in range(2)
        ]

    def row_edges(s):
        return copy_of(
            4 + 3 * (1 - s), s, sA.at[s, pl.ds(0, nq + 3)], rA.at[1 - s, pl.ds(0, nq + 3)]
        )

    def row_corners(s):
        return [
            copy_of(
                4 + 3 * (1 - s), 4 + 2 * s + t,
                sA.at[s, pl.ds(corner_at[t], 4)], rA.at[1 - s, pl.ds(corner_at[1 - t], 4)],
            )
            for t in range(2)
        ]

    def row_parts(s):
        return copy_of(5 + 3 * (1 - s), s, sRB.at[s], rRB.at[1 - s])

    def start(*those):
        for copy in those:
            copy.start()

    for copy in small:
        copy.wait()
    mass = mass_ref[...]
    x_at = lax.broadcasted_iota(jnp.int32, (nx, ny), 0)
    y_at = lax.broadcasted_iota(jnp.int32, (nx, ny), 1)
    zero_row, zero_col = jnp.zeros((1, ny), jnp.float32), jnp.zeros((nx, 1), jnp.float32)
    down = jnp.concatenate([zero_row, mass[: nx - 1]], axis=0)
    up = jnp.concatenate([mass[1:], zero_row], axis=0)
    mass = mass + jnp.where((x_at & 3) == 0, down, 0.0) + jnp.where((x_at & 3) == 3, up, 0.0)
    back = jnp.concatenate([zero_col, mass[:, : ny - 1]], axis=1)
    ahead = jnp.concatenate([mass[:, 1:], zero_col], axis=1)
    mass = mass + jnp.where((y_at & 3) == 0, back, 0.0) + jnp.where((y_at & 3) == 3, ahead, 0.0)
    cross = cross_ref[...]
    for slot, v in enumerate((diag_ref[:, 0, :], cross, diag_ref[:, 1, :], mass)):
        for ex in range(nbx):
            met[ex, 4 * slot:4 * slot + 4, :ny] = v[4 * ex:4 * ex + 4]

    sub = lax.broadcasted_iota(jnp.int32, tile, 0)
    halves_of = [pl.ds(8 * i, 8) for i in range(2)]

    half_lanes = 32

    def side_by_side(v, w):
        return jnp.where(lane < half_lanes, v, pltpu.roll(w, half_lanes, 1))

    for s in range(2):
        sM[s] = side_by_side(*[met[s * (nbx - 1), half, :] for half in halves_of])
    for t in range(2):
        packed = [jnp.zeros(tile, jnp.float32)] * 2
        for ex in range(nbx):
            for i, half in enumerate(halves_of):
                v = pltpu.roll(met[ex, half, :], (4 * ex - t * (ny - 4)) % lanes, 1)
                packed[i] = jnp.where((lane >= 4 * ex) & (lane < 4 * ex + 4), v, packed[i])
        sM[2 + t] = side_by_side(*packed)

    def inverted(ex, mass_of=lambda v: v):
        v = met[ex, halves_of[1], :]
        return jnp.where(sub < 4, v, 1.0 / mass_of(v))

    for ex in range(nbx):
        v, w = met[ex, halves_of[0], :], inverted(ex)
        for y in range(ny):
            B[ex, y, halves_of[0], :] = in_all_lanes(v, y)
            B[ex, y, halves_of[1], :] = in_all_lanes(w, y)

    def lift(v, to, at, lane_of):
        for i, y in enumerate(lane_of):
            for h, half in enumerate(halves_of):
                to[(*at, i, half)] = in_all_lanes(v, y + h * half_lanes)

    def rows_sum(src, x, *at):
        if x % 4 == 0 and x > 0:
            return src(x, *at) + src(x - 1, *at)
        if x % 4 == 3 and x < nx - 1:
            return src(x, *at) + src(x + 1, *at)
        return src(x, *at)

    def across(line):
        for ey in range(1, nby):
            v, w = line[2 * ey - 1], line[2 * ey]
            line[2 * ey - 1], line[2 * ey] = v + high * swap(w), w + low * swap(v)
        return line

    def in_W(x, q):
        return W[x, q]

    def first_laplacian(ex):
        for ey in range(nby):
            w = laplace(
                [[raw[4 * ex + a, 2 * ey + p] for p in range(2)] for a in range(4)],
                own_metrics(ex, ey),
            )
            for a in range(4):
                for p in range(2):
                    W[4 * ex + a, 2 * ey + p] = w(a, p)

    def first_rows(xs):
        for x in xs:
            if x % 4 == 0 and x > 0:
                continue
            line = across([rows_sum(in_W, x, q) for q in range(nq)])
            for q in range(nq):
                T[x, q] = line[q]
                if x % 4 == 3 and x < nx - 1:
                    T[x + 1, q] = line[q]

    def inner_first(xs):
        for x in xs:
            for q in range(nq):
                v = T[x, q] * inverse_mass(x, q)
                U[x, q] = high * v if q == 0 else low * v if q == nq - 1 else v

    def known_values(ex, ey):
        return [
            [None if x in (0, nx - 1) else U[x, 2 * ey + p] for p in range(2)]
            for x in range(4 * ex, 4 * ex + 4)
        ]

    def known_parts(ex):
        edge = {0: (0, 0), nbx - 1: (1, 3)}.get(ex)
        line = [None] * nq
        for ey in range(nby):
            if edge is None and 0 < ey < nby - 1:
                continue
            w = laplace(known_values(ex, ey), own_metrics(ex, ey))
            if edge:
                line[2 * ey], line[2 * ey + 1] = w(edge[1], 0), w(edge[1], 1)
            for t, e in ((0, 0), (1, nby - 1)):
                if ey == e:
                    for a in range(4):
                        side[t, 4 * ex + a] = w(a, t)
        if edge:
            line = across(line)
            for q in range(nq):
                sRB[edge[0], q] = line[q]

    def stage_row(s):
        xe, near = s * (nx - 1), (nx - 4 if s else 1)
        for q in range(nq):
            sA[s, q] = T[xe, q]
        for i in range(3):
            sA[s, nq + i] = jnp.where(is_low, T[near + i, 0], T[near + i, nq - 1])

    def stage_corner(s, t):
        xe, near, q = s * (nx - 1), (nx - 4 if s else 1), t * (nq - 1)
        for p in range(2):
            sA[s, corner_at[t] + p] = T[xe, t * (nq - 2) + p]
        halves = [T[near + i, q] for i in range(3)] + [sRB[s, q]]
        for i in range(2):
            sA[s, corner_at[t] + 2 + i] = pack_column(t, halves[2 * i], halves[2 * i + 1])

    def pack_column(t, v, w):
        return jnp.where(is_low, swap(v), w) if t else jnp.where(is_low, v, swap(w))

    def exchange(first, hold=False):
        near, far = (lambda s: s * (nbx - 1)), (lambda s: 1 + s * (nbx - 3))
        rows = [range(4), range(nx - 5, nx)]
        edge_rows = [range(1, 4), range(nx - 4, nx - 1)]
        other = 1 - first
        columns = [copy_of(0, 2 + t, sM.at[2 + t], rMc.at[1 - t]) for t in range(2)]
        waiting = []

        def launch(*those):
            if hold:
                waiting.extend(those)
            else:
                start(*those)

        first_laplacian(near(first))
        first_laplacian(far(first))
        first_rows(rows[first])
        stage_row(first)
        if not hold:
            pl.semaphore_wait(barrier, 8)
            if first:
                @pl.when(face == faces - 1)
                def _():
                    for k in after:
                        pl.semaphore_signal(late, inc=1, device_id=peers[k], device_id_type=MESH)
        launch(*row_metrics(first), row_edges(first), *columns)

        def known(s):
            inner_first(edge_rows[s])
            known_parts(near(s))
            for t in range(2):
                stage_corner(s, t)

        known(first)
        launch(*row_corners(first), row_parts(first))
        for ex in range(nbx):
            if ex not in (near(first), far(first)):
                first_laplacian(ex)
        first_rows(range(5, nx - 5))
        first_rows(rows[other])
        for t in range(2):
            q = t * (nq - 1)
            for k in range(nx // 2):
                sCA[t, k] = pack_column(t, T[2 * k, q], T[2 * k + 1, q])
            for s in range(2):
                for p in range(2):
                    sCA[t, nx // 2 + 2 * s + p] = T[s * (nx - 1), t * (nq - 2) + p]
            launch(copy_of(1, 2 + t, sCA.at[t], rCA.at[1 - t]))
        stage_row(other)
        known(other)
        inner_first(range(4, nx - 4))
        for ex in range(1, nbx - 1):
            known_parts(ex)
        for t in range(2):
            def in_side(x, t=t):
                return side[t, x]

            for k in range(nx // 2):
                sCB[t, k] = pack_column(t, rows_sum(in_side, 2 * k), rows_sum(in_side, 2 * k + 1))
            launch(copy_of(2, 2 + t, sCB.at[t], rCB.at[1 - t]))
        if hold:
            pl.semaphore_wait(barrier, 5)
            start(*waiting)
        else:
            start(*row_metrics(other), row_edges(other), *row_corners(other), row_parts(other))

    load.wait()

    @pl.when(face == 0)
    def _():
        exchange(1, hold=True)

    @pl.when((face > 0) & (face < faces // 2))
    def _():
        exchange(0)

    @pl.when(face >= faces // 2)
    def _():
        exchange(1)

    def turned(v, shift):
        return pltpu.roll(v, shift % lanes, 1)

    def mass_row(v, a):
        return wide(v[4 + a:5 + a, :])

    def at_ends(left, right):
        return jnp.where(lane == 0, left, 0.0) + jnp.where(lane == ny - 1, right, 0.0)

    def column_masses(t, ex):
        return turned(rMc[t], t * (ny - 1) - (half_lanes + 4 * ex + 3 * (1 - t)))

    def column_part(ref, t, x):
        v = ref[t, x // 2]
        if x % 2 != t:
            v = swap(v)
        return (high if t else low) * v

    def second_elements(ex, eys):
        for ey in eys:
            w = laplace(
                [[U[4 * ex + a, 2 * ey + p] for p in range(2)] for a in range(4)],
                own_metrics(ex, ey),
            )
            for a in range(4):
                for p in range(2):
                    W[4 * ex + a, 2 * ey + p] = w(a, p)

    def side_elements(t, ex, row=None, ext=None):
        u = []
        for a in range(4):
            v = swap(U[4 * ex + a, t * (nq - 1)])
            u.append([low * v, None] if t else [None, high * v])
        if row is not None:
            u[row] = ext
        w = laplace(u, metrics(Bc, t, ex))
        for a in range(4):
            side[t, 4 * ex + a] = w(a, 1 - t)

    inner = range(1, nby - 1)
    for ex in range(1, nbx - 1):
        second_elements(ex, inner)
    arrived(0, rMc)
    for ex in range(nbx):
        v = inverted(ex, lambda v: v + at_ends(column_masses(0, ex), column_masses(1, ex)))
        for y in (0, ny - 1):
            B[ex, y, halves_of[1], :] = in_all_lanes(v, y)
        for t in range(2):
            lift(rMc[t], Bc, (t, ex), range(4 * ex, 4 * ex + 4))
    arrived(1, rCA)
    for x in range(1, nx - 1):
        for t in range(2):
            q = t * (nq - 1)
            U[x, q] = (T[x, q] + column_part(rCA, t, x)) * inverse_mass(x, q)
    for ex in range(1, nbx - 1):
        second_elements(ex, (0, nby - 1))
        for t in range(2):
            side_elements(t, ex)

    @pl.when(face == 0)
    def _():
        pl.semaphore_wait(late, 3)
        start(*row_metrics(0), row_edges(0), *row_corners(0), row_parts(0))

    arrived(2, rCB)

    def summed(x, halo=None, corner=None):
        line = [rows_sum(in_W, x, q) for q in range(nq)]
        if halo:
            line = [add(v, h) for v, h in zip(line, halo)]
        line = across(line)
        for t in range(2):
            q = t * (nq - 1)
            v = rows_sum(lambda x: side[t, x], x)
            if corner:
                v = v + corner[t]
            v = swap(v)
            if corner:
                last = rA[s_of(x), corner_at[t] + 3]
                v = v + (last if t else swap(last))
            line[q] = line[q] + (high if t else low) * v + column_part(rCB, t, x)
        return line

    def s_of(x):
        return 0 if x == 0 else 1

    def finish(x):
        line = summed(x)
        for at in [x] + ([x + 1] if x % 4 == 3 and x < nx - 1 else []):
            for q in range(nq):
                out_ref[at, q] = line[q] * inverse_mass(at, q)

    for x in range(5, nx - 5):
        if x % 4:
            finish(x)

    def ring_metrics(s):
        ex, own_row, halo_row = s * (nbx - 1), 3 * s, 3 - 3 * s
        arrived(3 + 3 * s, rMr.at[s])
        beyond = [turned(rMr[s, k], -half_lanes) for k in range(3)]
        own = sub == 4 + own_row
        ends = [
            column_masses(t, ex)
            + jnp.where(own, mass_row(turned(beyond[1 + t], (2 * t - 1) * (ny - 1)), halo_row), 0.0)
            for t in range(2)
        ]
        v = inverted(ex, lambda v: (
            v + jnp.where(own, mass_row(beyond[0], halo_row), 0.0) + at_ends(*ends)
        ))
        for y in range(ny):
            B[ex, y, halves_of[1], :] = in_all_lanes(v, y)
        lift(rMr[s, 0], Br, (s,), range(ny))
        for t in range(2):
            lift(rMr[s, 1 + t], Bd, (2 * s + t,), range(4) if t else range(ny - 4, ny))
            v = 1.0 / (
                mass_row(turned(rMc[t], -(half_lanes + 4 * ex)), own_row)
                + mass_row(turned(beyond[1 + t], 0 if t else -(ny - 4)), halo_row)
            )
            for p in range(2):
                inv[s, 2 * t + p] = jnp.where(
                    is_low, in_all_lanes(v, 2 * p), in_all_lanes(v, 2 * p + 1)
                )
        v = 1.0 / (beyond[0] + at_ends(
            turned(beyond[1], -(ny - 1)), turned(beyond[2], ny - 1)
        ))
        for i in range(3):
            row = mass_row(v, i + s)
            inv[s, 4 + i] = jnp.where(is_low, in_all_lanes(row, 0), in_all_lanes(row, ny - 1))

    def ring_rows(s):
        xe, ex, own_row, halo_row = s * (nx - 1), s * (nbx - 1), 3 * s, 3 - 3 * s
        rest = [a for a in range(4) if a != halo_row]
        arrived(4 + 3 * s, rA.at[s])
        for q in range(nq):
            v = T[xe, q] + rA[s, q]
            for t in range(2):
                if q == t * (nq - 1):
                    v = v + column_part(rCA, t, xe)
                    v = v + (high if t else low) * swap(rA[s, corner_at[t] + 1 - t])
            U[xe, q] = v * inverse_mass(xe, q)
        ext = []
        for t in range(2):
            e = [
                (rCA[t, nx // 2 + 2 * s + p] + rA[s, corner_at[t] + p]) * inv[s, 2 * t + p]
                for p in range(2)
            ]
            corner = swap(U[xe, t * (nq - 1)])
            e[1 - t] = high * e[0] + low * corner if t else low * e[1] + high * corner
            ext.append(e)
        beyond = []
        for i in range(3):
            v, w = [rA[s, at + 2 + i // 2] for at in corner_at]
            v, w = (swap(v), w) if i % 2 else (v, swap(w))
            beyond.append((rA[s, nq + i] + low * v + high * w) * inv[s, 4 + i])

        second_elements(ex, range(nby))
        for t in range(2):
            side_elements(t, ex, own_row, ext[t])
        halo = []
        for ey in range(nby):
            u = [[None, None] for _ in range(4)]
            u[halo_row] = [U[xe, 2 * ey + p] for p in range(2)]
            for i, a in enumerate(rest):
                if ey == 0:
                    u[a][0] = low * beyond[i]
                if ey == nby - 1:
                    u[a][1] = high * beyond[i]
            w = laplace(u, functools.cache(lambda slot, a, p, ey=ey: tile_of(
                lambda j: Br[s, 4 * ey + j, 4 * slot + a:4 * slot + a + 1, :], p
            )))
            halo += [w(halo_row, 0), w(halo_row, 1)]
        corner = []
        for t in range(2):
            u = [[None, None] for _ in range(4)]
            u[halo_row] = ext[t]
            for i, a in enumerate(rest):
                v = swap(beyond[i])
                u[a] = [low * v, None] if t else [None, high * v]
            w = laplace(u, metrics(Bd, 2 * s + t))
            corner.append(w(halo_row, 1 - t))
        for x in (range(nx - 5, nx) if s else range(5)):
            if x % 4 and x != xe:
                finish(x)
        line = summed(xe, halo, corner)
        for q in range(nq):
            T[xe, q] = line[q]

    def last_row(s):
        xe = s * (nx - 1)
        arrived(5 + 3 * s, rRB.at[s])
        for q in range(nq):
            out_ref[xe, q] = (T[xe, q] + rRB[s, q]) * inverse_mass(xe, q)


    ring_metrics(1)

    @pl.when(face != 0)
    def _():
        ring_metrics(0)

    ring_rows(1)

    @pl.when(face == 0)
    def _():
        ring_metrics(0)

    ring_rows(0)
    last_row(1)
    last_row(0)
    pltpu.make_async_remote_copy(
        src_ref=sent, dst_ref=sent, send_sem=send_sem, recv_sem=recv_sem.at[0],
        device_id=peers[0], device_id_type=MESH,
    ).wait_send()


def solution(mesh):
    faces, cols = mesh.shape["face"], mesh.shape["col"]

    def shards(fields, metric_diag, metric_cross, point_mass):
        nf, nx, ny, lanes = fields.shape
        nbx, nby = nx // 4, ny // 4
        nq = ny // 2
        f32 = jnp.float32
        tiles = (nx, nq, 2 * nf, lanes)

        def vmem(*shape):
            return pltpu.VMEM(shape, f32)

        def messages():
            return [
                vmem(2, nq + 3 + 8, 2 * nf, lanes),
                vmem(2, nq, 2 * nf, lanes),
                vmem(2, nx // 2 + 4, 2 * nf, lanes),
                vmem(2, nx // 2, 2 * nf, lanes),
            ]

        tiles_sent = 2 * (2 * nq + 3 + 4) + 2 * (nx + 4) + 8 + 8
        out = pl.pallas_call(
            functools.partial(kernel, faces, cols, nf, nbx, nby),
            out_shape=jax.ShapeDtypeStruct(tiles, f32),
            in_specs=[pl.BlockSpec(memory_space=pltpu.HBM)] * 4,
            out_specs=pl.BlockSpec(memory_space=pltpu.VMEM),
            scratch_shapes=[
                vmem(nx, 2, ny),
                vmem(nx, ny),
                vmem(nx, ny),
                vmem(*tiles),
                vmem(*tiles),
                vmem(*tiles),
                vmem(*tiles),
                vmem(2, nx, 2 * nf, lanes),
                vmem(nbx, 16, lanes),
                vmem(nbx, ny, 16, lanes),
                vmem(2, ny, 16, lanes),
                vmem(2, nbx, 4, 16, lanes),
                vmem(4, 4, 16, lanes),
                vmem(2, 7, 2 * nf, lanes),
                vmem(4, 2 * nf, lanes),
                *messages(),
                vmem(2, 2 * nf, lanes),
                vmem(2, 3, 2 * nf, lanes),
                *messages(),
                vmem(tiles_sent, 2 * nf, lanes),
                pltpu.SemaphoreType.DMA((3,)),
                pltpu.SemaphoreType.DMA,
                pltpu.SemaphoreType.DMA,
                pltpu.SemaphoreType.DMA((9,)),
                pltpu.SemaphoreType.REGULAR,
            ],
            compiler_params=pltpu.CompilerParams(
                collective_id=0, has_side_effects=True, vmem_limit_bytes=32 * 1024 * 1024
            ),
        )(*[
            pltpu.with_memory_space_constraint(v, pltpu.HBM)
            for v in (
                fields.transpose(1, 2, 0, 3).reshape(tiles),
                metric_diag.transpose(1, 0, 2), metric_cross, point_mass,
            )
        ])
        return out.reshape(nx, ny, nf, lanes).transpose(2, 0, 1, 3)

    return jax.shard_map(
        shards,
        mesh=mesh,
        in_specs=(
            P(None, "face", "col", None),
            P(None, "face", "col"),
            P("face", "col"),
            P("face", "col"),
        ),
        out_specs=P(None, "face", "col", None),
        check_vma=False,
    )
```

```python
import functools

import jax
import jax.numpy as jnp
import numpy as np
from jax import lax
from jax.experimental import pallas as pl
from jax.experimental.pallas import tpu as pltpu
from jax.sharding import PartitionSpec as P

MESH = pl.DeviceIdType.MESH


def derivative_table():
    small = 1.0 / np.sqrt(5.0)
    nodes = np.array([-1.0, -small, small, 1.0])
    count = nodes.shape[0]
    weights = np.array(
        [np.prod([nodes[a] - nodes[k] for k in range(count) if k != a]) for a in range(count)]
    )
    table = np.zeros((count, count))
    for a in range(count):
        for b in range(count):
            if a == b:
                table[a, b] = np.sum([1.0 / (nodes[a] - nodes[k]) for k in range(count) if k != a])
            else:
                table[a, b] = weights[a] / weights[b] / (nodes[a] - nodes[b])
    return [[float(np.float32(v)) for v in row] for row in table]


def add(a, b):
    if a is None or b is None:
        return b if a is None else a
    return a + b


def mul(a, b):
    return None if b is None else a * b


def combine(coefs, terms):
    total = None
    for c, t in zip(coefs, terms):
        if isinstance(c, float) and c == 0.0:
            continue
        total = add(total, mul(c, t))
    return total


def kernel(
    faces, cols, nf, nbx, nby,
    fields_hbm, diag_hbm, cross_hbm, mass_hbm, out_ref,
    diag_ref, cross_ref, mass_ref, raw, U, W, T, side, met, B, Br, Bc, Bd, inv,
    sM, sA, sRB, sCA, sCB, rMc, rMr, rA, rRB, rCA, rCB, sent,
    small_sem, load_sem, send_sem, recv_sem, late,
):
    face, col = lax.axis_index("face"), lax.axis_index("col")
    fside = (lax.rem(face + faces - 1, faces), lax.rem(face + 1, faces))
    cside = (lax.rem(col + cols - 1, cols), lax.rem(col + 1, cols))
    peers = [(fside[0], col), (fside[1], col), (face, cside[0]), (face, cside[1])]
    peers += [(fside[s], cside[t]) for s in range(2) for t in range(2)]
    opposite = [1, 0, 3, 2, 7, 6, 5, 4]
    before, after = [0, 4, 5], [1, 6, 7]

    barrier = pltpu.get_barrier_semaphore()
    for k in (2, 3):
        pl.semaphore_signal(barrier, inc=1, device_id=peers[k], device_id_type=MESH)
    for on_time, those in (((face < 1) | (face > 2), before), (face != faces - 1, after)):
        @pl.when(on_time)
        def _():
            for k in those:
                pl.semaphore_signal(barrier, inc=1, device_id=peers[k], device_id_type=MESH)

    nx, ny, nq = 4 * nbx, 4 * nby, 2 * nby
    lanes = raw.shape[-1]
    tile = (2 * nf, lanes)
    corner_at = [nq + 3, nq + 7]
    small = [
        pltpu.make_async_copy(src, dst, small_sem.at[k])
        for k, (src, dst) in enumerate(
            ((diag_hbm, diag_ref), (cross_hbm, cross_ref), (mass_hbm, mass_ref))
        )
    ]
    load = pltpu.make_async_copy(fields_hbm, raw, load_sem)
    for copy in small:
        copy.start()
    load.start()

    D = derivative_table()
    is_low = lax.broadcasted_iota(jnp.int32, tile, 0) < nf
    lane = lax.broadcasted_iota(jnp.int32, tile, 1)
    low = jnp.where(is_low, 1.0, 0.0)
    high = 1.0 - low

    def swap(v):
        return pltpu.roll(v, nf, 0)

    def halves(table):
        return [
            [
                jnp.where(is_low, table[2 * p][2 * q + k], table[2 * p + 1][2 * q + 1 - k])
                for q in range(2) for k in range(2)
            ]
            for p in range(2)
        ]

    minus_t = [[-D[b][a] for b in range(4)] for a in range(4)]
    D_half, minus_half = halves(D), halves(minus_t)

    def mixed(v, w):
        return [v, None if v is None else swap(v), w, None if w is None else swap(w)]

    def laplace(u, m):
        @functools.cache
        def mix(a):
            return mixed(*u[a])

        @functools.cache
        def flux(a, p):
            gx = combine(D[a], [u[b][p] for b in range(4)])
            gy = combine(D_half[p], mix(a))
            return gx, gy

        @functools.cache
        def fx(a, p):
            gx, gy = flux(a, p)
            return add(
                None if gx is None else m(0, a, p) * gx, None if gy is None else m(1, a, p) * gy
            )

        @functools.cache
        def mix_fy(a):
            parts = []
            for p in range(2):
                gx, gy = flux(a, p)
                parts.append(add(
                    None if gx is None else m(1, a, p) * gx, None if gy is None else m(2, a, p) * gy
                ))
            return mixed(*parts)

        def w(a, p):
            return add(
                combine(minus_t[a], [fx(b, p) for b in range(4)]), combine(minus_half[p], mix_fy(a))
            )

        return w

    def wide(row):
        return jnp.broadcast_to(row, tile)

    def in_all_lanes(v, y):
        return jnp.broadcast_to(v[:, y:y + 1], tile)

    def tile_of(column, p):
        return jnp.where(is_low, wide(column(2 * p)), wide(column(2 * p + 1)))

    def metrics(ref, *at):
        return functools.cache(
            lambda slot, a, p: tile_of(lambda j: ref[(*at, j, pl.ds(4 * slot + a, 1))], p)
        )

    def own_metrics(ex, ey):
        return functools.cache(lambda slot, a, p: tile_of(
            lambda j: B[ex, 4 * ey + j, 4 * slot + a:4 * slot + a + 1, :], p
        ))

    def inverse_mass(x, q):
        return own_metrics(x // 4, q // 2)(3, x % 4, q % 2)

    def copy_of(group, k, src, dst):
        return pltpu.make_async_remote_copy(
            src_ref=src, dst_ref=dst, send_sem=send_sem, recv_sem=recv_sem.at[group],
            device_id=peers[k], device_id_type=MESH,
        )

    def arrived(group, landed):
        pltpu.make_async_remote_copy(
            src_ref=landed, dst_ref=landed, send_sem=send_sem, recv_sem=recv_sem.at[group],
            device_id=peers[0], device_id_type=MESH,
        ).wait_recv()

    def row_metrics(s):
        return [copy_of(3 + 3 * (1 - s), s, sM.at[s], rMr.at[1 - s, 0])] + [
            copy_of(3 + 3 * (1 - s), 4 + 2 * s + t, sM.at[s], rMr.at[1 - s, 2 - t]) for t in range(2)
        ]

    def row_edges(s, at, size):
        return copy_of(4 + 3 * (1 - s), s, sA.at[s, pl.ds(at, size)], rA.at[1 - s, pl.ds(at, size)])

    def row_corners(s):
        return [
            copy_of(
                4 + 3 * (1 - s), 4 + 2 * s + t,
                sA.at[s, pl.ds(corner_at[t], 4)], rA.at[1 - s, pl.ds(corner_at[1 - t], 4)],
            )
            for t in range(2)
        ]

    def row_parts(s):
        return copy_of(5 + 3 * (1 - s), s, sRB.at[s], rRB.at[1 - s])

    def all_to(s):
        return [*row_metrics(s), row_edges(s, 0, nq + 3), *row_corners(s), row_parts(s)]

    def start(*those):
        for copy in those:
            copy.start()

    for copy in small:
        copy.wait()
    mass = mass_ref[...]
    x_at = lax.broadcasted_iota(jnp.int32, (nx, ny), 0)
    y_at = lax.broadcasted_iota(jnp.int32, (nx, ny), 1)
    zero_row, zero_col = jnp.zeros((1, ny), jnp.float32), jnp.zeros((nx, 1), jnp.float32)
    down = jnp.concatenate([zero_row, mass[: nx - 1]], axis=0)
    up = jnp.concatenate([mass[1:], zero_row], axis=0)
    mass = mass + jnp.where((x_at & 3) == 0, down, 0.0) + jnp.where((x_at & 3) == 3, up, 0.0)
    back = jnp.concatenate([zero_col, mass[:, : ny - 1]], axis=1)
    ahead = jnp.concatenate([mass[:, 1:], zero_col], axis=1)
    mass = mass + jnp.where((y_at & 3) == 0, back, 0.0) + jnp.where((y_at & 3) == 3, ahead, 0.0)
    cross = cross_ref[...]
    for slot, v in enumerate((diag_ref[:, 0, :], cross, diag_ref[:, 1, :], mass)):
        for ex in range(nbx):
            met[ex, 4 * slot:4 * slot + 4, :ny] = v[4 * ex:4 * ex + 4]

    sub = lax.broadcasted_iota(jnp.int32, tile, 0)
    halves_of = [pl.ds(8 * i, 8) for i in range(2)]

    half_lanes = 32

    def side_by_side(v, w):
        return jnp.where(lane < half_lanes, v, pltpu.roll(w, half_lanes, 1))

    for s in range(2):
        sM[s] = side_by_side(*[met[s * (nbx - 1), half, :] for half in halves_of])
    for t in range(2):
        packed = [jnp.zeros(tile, jnp.float32)] * 2
        for ex in range(nbx):
            for i, half in enumerate(halves_of):
                v = pltpu.roll(met[ex, half, :], (4 * ex - t * (ny - 4)) % lanes, 1)
                packed[i] = jnp.where((lane >= 4 * ex) & (lane < 4 * ex + 4), v, packed[i])
        sM[2 + t] = side_by_side(*packed)

    def inverted(ex, mass_of=lambda v: v):
        v = met[ex, halves_of[1], :]
        return jnp.where(sub < 4, v, 1.0 / mass_of(v))

    def lift_own(ex):
        v, w = met[ex, halves_of[0], :], inverted(ex)
        for y in range(ny):
            B[ex, y, halves_of[0], :] = in_all_lanes(v, y)
            B[ex, y, halves_of[1], :] = in_all_lanes(w, y)

    def lift(v, to, at, lane_of):
        for i, y in enumerate(lane_of):
            for h, half in enumerate(halves_of):
                to[(*at, i, half)] = in_all_lanes(v, y + h * half_lanes)

    def rows_sum(src, x, *at):
        if x % 4 == 0 and x > 0:
            return src(x, *at) + src(x - 1, *at)
        if x % 4 == 3 and x < nx - 1:
            return src(x, *at) + src(x + 1, *at)
        return src(x, *at)

    def across(line):
        for ey in range(1, nby):
            v, w = line[2 * ey - 1], line[2 * ey]
            line[2 * ey - 1], line[2 * ey] = v + high * swap(w), w + low * swap(v)
        return line

    def in_W(x, q):
        return W[x, q]

    def first_laplacian(ex):
        lift_own(ex)
        for ey in range(nby):
            w = laplace(
                [[raw[4 * ex + a, 2 * ey + p] for p in range(2)] for a in range(4)],
                own_metrics(ex, ey),
            )
            for a in range(4):
                for p in range(2):
                    W[4 * ex + a, 2 * ey + p] = w(a, p)

    def first_rows(xs):
        for x in xs:
            if x % 4 == 0 and x > 0:
                continue
            line = across([rows_sum(in_W, x, q) for q in range(nq)])
            for q in range(nq):
                T[x, q] = line[q]
                if x % 4 == 3 and x < nx - 1:
                    T[x + 1, q] = line[q]

    def inner_first(xs):
        for x in xs:
            for q in range(nq):
                v = T[x, q] * inverse_mass(x, q)
                U[x, q] = high * v if q == 0 else low * v if q == nq - 1 else v

    def known_values(ex, ey):
        return [
            [None if x in (0, nx - 1) else U[x, 2 * ey + p] for p in range(2)]
            for x in range(4 * ex, 4 * ex + 4)
        ]

    def known_parts(ex):
        edge = {0: (0, 0), nbx - 1: (1, 3)}.get(ex)
        line = [None] * nq
        for ey in range(nby):
            if edge is None and 0 < ey < nby - 1:
                continue
            w = laplace(known_values(ex, ey), own_metrics(ex, ey))
            if edge:
                line[2 * ey], line[2 * ey + 1] = w(edge[1], 0), w(edge[1], 1)
            for t, e in ((0, 0), (1, nby - 1)):
                if ey == e:
                    for a in range(4):
                        side[t, 4 * ex + a] = w(a, t)
        if edge:
            line = across(line)
            for q in range(nq):
                sRB[edge[0], q] = line[q]

    def stage_edge(s):
        for q in range(nq):
            sA[s, q] = T[s * (nx - 1), q]

    def stage_corner(s, t):
        xe, near, q = s * (nx - 1), (nx - 4 if s else 1), t * (nq - 1)
        for p in range(2):
            sA[s, corner_at[t] + p] = T[xe, t * (nq - 2) + p]
        if t == 0:
            for i in range(3):
                sA[s, nq + i] = jnp.where(is_low, T[near + i, 0], T[near + i, nq - 1])
        halves = [T[near + i, q] for i in range(3)] + [sRB[s, q]]
        for i in range(2):
            sA[s, corner_at[t] + 2 + i] = pack_column(t, halves[2 * i], halves[2 * i + 1])

    def pack_column(t, v, w):
        return jnp.where(is_low, swap(v), w) if t else jnp.where(is_low, v, swap(w))

    def exchange(first, hold=False):
        near, far = (lambda s: s * (nbx - 1)), (lambda s: 1 + s * (nbx - 3))
        rows = [range(3), range(nx - 3, nx)]
        pair = [3, nx - 5]
        edge_rows = [range(1, 4), range(nx - 4, nx - 1)]
        other = 1 - first
        columns = [copy_of(0, 2 + t, sM.at[2 + t], rMc.at[1 - t]) for t in range(2)]

        first_laplacian(near(first))
        first_rows(rows[first])
        stage_edge(first)
        if not hold:
            pl.semaphore_wait(barrier, 8 if first else jnp.where(face == 1, 5, 8))
            start(*row_metrics(first), row_edges(first, 0, nq), *columns)
            are_late, those = ((face <= 2, before), (face == faces - 1, after))[first]

            @pl.when(are_late)
            def _():
                for k in those:
                    pl.semaphore_signal(
                        late.at[1 - first], inc=1, device_id=peers[k], device_id_type=MESH
                    )

        first_laplacian(far(first))
        first_rows([pair[first]])

        def known(s):
            inner_first(edge_rows[s])
            known_parts(near(s))
            for t in range(2):
                stage_corner(s, t)

        known(first)
        if not hold:
            start(row_edges(first, nq, 3), *row_corners(first), row_parts(first))
        for ex in range(nbx):
            if ex not in (near(first), far(first)):
                first_laplacian(ex)
        first_rows(range(5, nx - 5))
        first_rows([*rows[other], pair[other]])
        if hold:
            pl.semaphore_wait(barrier, 2)
            start(*columns)
        for t in range(2):
            q = t * (nq - 1)
            for k in range(nx // 2):
                sCA[t, k] = pack_column(t, T[2 * k, q], T[2 * k + 1, q])
            for s in range(2):
                for p in range(2):
                    sCA[t, nx // 2 + 2 * s + p] = T[s * (nx - 1), t * (nq - 2) + p]
            start(copy_of(1, 2 + t, sCA.at[t], rCA.at[1 - t]))
        def to_other(*those):
            if other:
                @pl.when(face > 1)
                def _():
                    start(*those)
            elif not hold:
                start(*those)

        stage_edge(other)
        to_other(*row_metrics(other), row_edges(other, 0, nq))
        known(other)
        to_other(row_edges(other, nq, 3), *row_corners(other), row_parts(other))
        inner_first(range(4, nx - 4))
        for ex in range(1, nbx - 1):
            known_parts(ex)
        for t in range(2):
            def in_side(x, t=t):
                return side[t, x]

            for k in range(nx // 2):
                sCB[t, k] = pack_column(t, rows_sum(in_side, 2 * k), rows_sum(in_side, 2 * k + 1))
            start(copy_of(2, 2 + t, sCB.at[t], rCB.at[1 - t]))
        if other:
            @pl.when(face == 1)
            def _():
                pl.semaphore_wait(late.at[1], 3)
                start(*all_to(1))

    load.wait()

    @pl.when(face == 0)
    def _():
        exchange(1, hold=True)

    @pl.when((face > 0) & (face < faces - 1))
    def _():
        exchange(0)

    @pl.when(face >= faces - 1)
    def _():
        exchange(1)

    def turned(v, shift):
        return pltpu.roll(v, shift % lanes, 1)

    def mass_row(v, a):
        return wide(v[4 + a:5 + a, :])

    def at_ends(left, right):
        return jnp.where(lane == 0, left, 0.0) + jnp.where(lane == ny - 1, right, 0.0)

    def column_masses(t, ex):
        return turned(rMc[t], t * (ny - 1) - (half_lanes + 4 * ex + 3 * (1 - t)))

    def column_part(ref, t, x):
        v = ref[t, x // 2]
        if x % 2 != t:
            v = swap(v)
        return (high if t else low) * v

    def second_elements(ex, eys):
        for ey in eys:
            w = laplace(
                [[U[4 * ex + a, 2 * ey + p] for p in range(2)] for a in range(4)],
                own_metrics(ex, ey),
            )
            for a in range(4):
                for p in range(2):
                    W[4 * ex + a, 2 * ey + p] = w(a, p)

    def side_elements(t, ex, row=None, ext=None):
        u = []
        for a in range(4):
            v = swap(U[4 * ex + a, t * (nq - 1)])
            u.append([low * v, None] if t else [None, high * v])
        if row is not None:
            u[row] = ext
        w = laplace(u, metrics(Bc, t, ex))
        for a in range(4):
            side[t, 4 * ex + a] = w(a, 1 - t)

    inner = range(1, nby - 1)
    for ex in range(1, nbx - 1):
        second_elements(ex, inner)
    arrived(0, rMc)
    for ex in range(nbx):
        v = inverted(ex, lambda v: v + at_ends(column_masses(0, ex), column_masses(1, ex)))
        for y in (0, ny - 1):
            B[ex, y, halves_of[1], :] = in_all_lanes(v, y)
        for t in range(2):
            lift(rMc[t], Bc, (t, ex), range(4 * ex, 4 * ex + 4))
    arrived(1, rCA)
    for x in range(1, nx - 1):
        for t in range(2):
            q = t * (nq - 1)
            U[x, q] = (T[x, q] + column_part(rCA, t, x)) * inverse_mass(x, q)
    for ex in range(1, nbx - 1):
        second_elements(ex, (0, nby - 1))
        for t in range(2):
            side_elements(t, ex)

    @pl.when(face == 0)
    def _():
        pl.semaphore_wait(late.at[1], 3)
        start(*all_to(1))
        pl.semaphore_wait(late.at[0], 3)
        start(*all_to(0))

    arrived(2, rCB)

    def summed(x, halo=None, corner=None):
        line = [rows_sum(in_W, x, q) for q in range(nq)]
        if halo:
            line = [add(v, h) for v, h in zip(line, halo)]
        line = across(line)
        for t in range(2):
            q = t * (nq - 1)
            v = rows_sum(lambda x: side[t, x], x)
            if corner:
                v = v + corner[t]
            v = swap(v)
            if corner:
                last = rA[s_of(x), corner_at[t] + 3]
                v = v + (last if t else swap(last))
            line[q] = line[q] + (high if t else low) * v + column_part(rCB, t, x)
        return line

    def s_of(x):
        return 0 if x == 0 else 1

    def finish(x):
        line = summed(x)
        for at in [x] + ([x + 1] if x % 4 == 3 and x < nx - 1 else []):
            for q in range(nq):
                out_ref[at, q] = line[q] * inverse_mass(at, q)

    for x in range(5, nx - 5):
        if x % 4:
            finish(x)

    def ring_metrics(s):
        ex, own_row, halo_row = s * (nbx - 1), 3 * s, 3 - 3 * s
        arrived(3 + 3 * s, rMr.at[s])
        beyond = [turned(rMr[s, k], -half_lanes) for k in range(3)]
        own = sub == 4 + own_row
        ends = [
            column_masses(t, ex)
            + jnp.where(own, mass_row(turned(beyond[1 + t], (2 * t - 1) * (ny - 1)), halo_row), 0.0)
            for t in range(2)
        ]
        v = inverted(ex, lambda v: (
            v + jnp.where(own, mass_row(beyond[0], halo_row), 0.0) + at_ends(*ends)
        ))
        for y in range(ny):
            B[ex, y, halves_of[1], :] = in_all_lanes(v, y)
        lift(rMr[s, 0], Br, (s,), range(ny))
        for t in range(2):
            lift(rMr[s, 1 + t], Bd, (2 * s + t,), range(4) if t else range(ny - 4, ny))
            v = 1.0 / (
                mass_row(turned(rMc[t], -(half_lanes + 4 * ex)), own_row)
                + mass_row(turned(beyond[1 + t], 0 if t else -(ny - 4)), halo_row)
            )
            for p in range(2):
                inv[s, 2 * t + p] = jnp.where(
                    is_low, in_all_lanes(v, 2 * p), in_all_lanes(v, 2 * p + 1)
                )
        v = 1.0 / (beyond[0] + at_ends(
            turned(beyond[1], -(ny - 1)), turned(beyond[2], ny - 1)
        ))
        for i in range(3):
            row = mass_row(v, i + s)
            inv[s, 4 + i] = jnp.where(is_low, in_all_lanes(row, 0), in_all_lanes(row, ny - 1))

    def ring_rows(s):
        xe, ex, own_row, halo_row = s * (nx - 1), s * (nbx - 1), 3 * s, 3 - 3 * s
        rest = [a for a in range(4) if a != halo_row]
        arrived(4 + 3 * s, rA.at[s])
        for q in range(nq):
            v = T[xe, q] + rA[s, q]
            for t in range(2):
                if q == t * (nq - 1):
                    v = v + column_part(rCA, t, xe)
                    v = v + (high if t else low) * swap(rA[s, corner_at[t] + 1 - t])
            U[xe, q] = v * inverse_mass(xe, q)
        ext = []
        for t in range(2):
            e = [
                (rCA[t, nx // 2 + 2 * s + p] + rA[s, corner_at[t] + p]) * inv[s, 2 * t + p]
                for p in range(2)
            ]
            corner = swap(U[xe, t * (nq - 1)])
            e[1 - t] = high * e[0] + low * corner if t else low * e[1] + high * corner
            ext.append(e)
        beyond = []
        for i in range(3):
            v, w = [rA[s, at + 2 + i // 2] for at in corner_at]
            v, w = (swap(v), w) if i % 2 else (v, swap(w))
            beyond.append((rA[s, nq + i] + low * v + high * w) * inv[s, 4 + i])

        second_elements(ex, range(nby))
        for t in range(2):
            side_elements(t, ex, own_row, ext[t])
        halo = []
        for ey in range(nby):
            u = [[None, None] for _ in range(4)]
            u[halo_row] = [U[xe, 2 * ey + p] for p in range(2)]
            for i, a in enumerate(rest):
                if ey == 0:
                    u[a][0] = low * beyond[i]
                if ey == nby - 1:
                    u[a][1] = high * beyond[i]
            w = laplace(u, functools.cache(lambda slot, a, p, ey=ey: tile_of(
                lambda j: Br[s, 4 * ey + j, 4 * slot + a:4 * slot + a + 1, :], p
            )))
            halo += [w(halo_row, 0), w(halo_row, 1)]
        corner = []
        for t in range(2):
            u = [[None, None] for _ in range(4)]
            u[halo_row] = ext[t]
            for i, a in enumerate(rest):
                v = swap(beyond[i])
                u[a] = [low * v, None] if t else [None, high * v]
            w = laplace(u, metrics(Bd, 2 * s + t))
            corner.append(w(halo_row, 1 - t))
        for x in (range(nx - 5, nx) if s else range(5)):
            if x % 4 and x != xe:
                finish(x)
        line = summed(xe, halo, corner)
        for q in range(nq):
            T[xe, q] = line[q]

    def last_row(s):
        xe = s * (nx - 1)
        arrived(5 + 3 * s, rRB.at[s])
        for q in range(nq):
            out_ref[xe, q] = (T[xe, q] + rRB[s, q]) * inverse_mass(xe, q)


    ring_metrics(1)

    @pl.when(face != 0)
    def _():
        ring_metrics(0)

    ring_rows(1)

    @pl.when(face == 0)
    def _():
        ring_metrics(0)

    ring_rows(0)
    last_row(1)
    last_row(0)
    pltpu.make_async_remote_copy(
        src_ref=sent, dst_ref=sent, send_sem=send_sem, recv_sem=recv_sem.at[0],
        device_id=peers[0], device_id_type=MESH,
    ).wait_send()


def solution(mesh):
    faces, cols = mesh.shape["face"], mesh.shape["col"]

    def shards(fields, metric_diag, metric_cross, point_mass):
        nf, nx, ny, lanes = fields.shape
        nbx, nby = nx // 4, ny // 4
        nq = ny // 2
        f32 = jnp.float32
        tiles = (nx, nq, 2 * nf, lanes)

        def vmem(*shape):
            return pltpu.VMEM(shape, f32)

        def messages():
            return [
                vmem(2, nq + 3 + 8, 2 * nf, lanes),
                vmem(2, nq, 2 * nf, lanes),
                vmem(2, nx // 2 + 4, 2 * nf, lanes),
                vmem(2, nx // 2, 2 * nf, lanes),
            ]

        tiles_sent = 2 * (2 * nq + 3 + 4) + 2 * (nx + 4) + 8 + 8
        out = pl.pallas_call(
            functools.partial(kernel, faces, cols, nf, nbx, nby),
            out_shape=jax.ShapeDtypeStruct(tiles, f32),
            in_specs=[pl.BlockSpec(memory_space=pltpu.HBM)] * 4,
            out_specs=pl.BlockSpec(memory_space=pltpu.VMEM),
            scratch_shapes=[
                vmem(nx, 2, ny),
                vmem(nx, ny),
                vmem(nx, ny),
                vmem(*tiles),
                vmem(*tiles),
                vmem(*tiles),
                vmem(*tiles),
                vmem(2, nx, 2 * nf, lanes),
                vmem(nbx, 16, lanes),
                vmem(nbx, ny, 16, lanes),
                vmem(2, ny, 16, lanes),
                vmem(2, nbx, 4, 16, lanes),
                vmem(4, 4, 16, lanes),
                vmem(2, 7, 2 * nf, lanes),
                vmem(4, 2 * nf, lanes),
                *messages(),
                vmem(2, 2 * nf, lanes),
                vmem(2, 3, 2 * nf, lanes),
                *messages(),
                vmem(tiles_sent, 2 * nf, lanes),
                pltpu.SemaphoreType.DMA((3,)),
                pltpu.SemaphoreType.DMA,
                pltpu.SemaphoreType.DMA,
                pltpu.SemaphoreType.DMA((9,)),
                pltpu.SemaphoreType.REGULAR((2,)),
            ],
            compiler_params=pltpu.CompilerParams(
                collective_id=0, has_side_effects=True, vmem_limit_bytes=32 * 1024 * 1024
            ),
        )(*[
            pltpu.with_memory_space_constraint(v, pltpu.HBM)
            for v in (
                fields.transpose(1, 2, 0, 3).reshape(tiles),
                metric_diag.transpose(1, 0, 2), metric_cross, point_mass,
            )
        ])
        return out.reshape(nx, ny, nf, lanes).transpose(2, 0, 1, 3)

    return jax.shard_map(
        shards,
        mesh=mesh,
        in_specs=(
            P(None, "face", "col", None),
            P(None, "face", "col"),
            P("face", "col"),
            P("face", "col"),
        ),
        out_specs=P(None, "face", "col", None),
        check_vma=False,
    )
```

```python
import functools

import jax
import jax.numpy as jnp
import numpy as np
from jax import lax
from jax.experimental import pallas as pl
from jax.experimental.pallas import tpu as pltpu
from jax.sharding import PartitionSpec as P

MESH = pl.DeviceIdType.MESH


def derivative_table():
    small = 1.0 / np.sqrt(5.0)
    nodes = np.array([-1.0, -small, small, 1.0])
    count = nodes.shape[0]
    weights = np.array(
        [np.prod([nodes[a] - nodes[k] for k in range(count) if k != a]) for a in range(count)]
    )
    table = np.zeros((count, count))
    for a in range(count):
        for b in range(count):
            if a == b:
                table[a, b] = np.sum([1.0 / (nodes[a] - nodes[k]) for k in range(count) if k != a])
            else:
                table[a, b] = weights[a] / weights[b] / (nodes[a] - nodes[b])
    return [[float(np.float32(v)) for v in row] for row in table]


def add(a, b):
    if a is None or b is None:
        return b if a is None else a
    return a + b


def mul(a, b):
    return None if b is None else a * b


def combine(coefs, terms):
    total = None
    for c, t in zip(coefs, terms):
        if isinstance(c, float) and c == 0.0:
            continue
        total = add(total, mul(c, t))
    return total


def kernel(
    faces, cols, nf, nbx, nby,
    fields_hbm, diag_hbm, cross_hbm, mass_hbm, out_ref,
    diag_ref, cross_ref, mass_ref, raw, U, W, T, side, met, B, Br, Bc, Bd, inv,
    sM, sMd, sA, sRB, sCA, sCB, rMc, rMr, rMd, rA, rRB, rCA, rCB, sent,
    small_sem, load_sem, send_sem, recv_sem, late,
):
    face, col = lax.axis_index("face"), lax.axis_index("col")
    fside = (lax.rem(face + faces - 1, faces), lax.rem(face + 1, faces))
    cside = (lax.rem(col + cols - 1, cols), lax.rem(col + 1, cols))
    peers = [(fside[0], col), (fside[1], col), (face, cside[0]), (face, cside[1])]
    peers += [(fside[s], cside[t]) for s in range(2) for t in range(2)]
    opposite = [1, 0, 3, 2, 7, 6, 5, 4]
    before, after = [0, 4, 5], [1, 6, 7]

    barrier = pltpu.get_barrier_semaphore()
    for k in (2, 3):
        pl.semaphore_signal(barrier, inc=1, device_id=peers[k], device_id_type=MESH)
    for on_time, those in (((face < 1) | (face > 2), before), (face != faces - 1, after)):
        @pl.when(on_time)
        def _():
            for k in those:
                pl.semaphore_signal(barrier, inc=1, device_id=peers[k], device_id_type=MESH)

    nx, ny, nq = 4 * nbx, 4 * nby, 2 * nby
    lanes = raw.shape[-1]
    tile = (2 * nf, lanes)
    corner_at = [nq + 3, nq + 7]
    small = [
        pltpu.make_async_copy(src, dst, small_sem.at[k])
        for k, (src, dst) in enumerate(
            ((diag_hbm, diag_ref), (cross_hbm, cross_ref), (mass_hbm, mass_ref))
        )
    ]
    load = pltpu.make_async_copy(fields_hbm, raw, load_sem)
    for copy in small:
        copy.start()
    load.start()

    D = derivative_table()
    is_low = lax.broadcasted_iota(jnp.int32, tile, 0) < nf
    lane = lax.broadcasted_iota(jnp.int32, tile, 1)
    low = jnp.where(is_low, 1.0, 0.0)
    high = 1.0 - low

    def swap(v):
        return pltpu.roll(v, nf, 0)

    def halves(table):
        return [
            [
                jnp.where(is_low, table[2 * p][2 * q + k], table[2 * p + 1][2 * q + 1 - k])
                for q in range(2) for k in range(2)
            ]
            for p in range(2)
        ]

    minus_t = [[-D[b][a] for b in range(4)] for a in range(4)]
    D_half, minus_half = halves(D), halves(minus_t)

    def mixed(v, w):
        return [v, None if v is None else swap(v), w, None if w is None else swap(w)]

    def laplace(u, m):
        @functools.cache
        def mix(a):
            return mixed(*u[a])

        @functools.cache
        def flux(a, p):
            gx = combine(D[a], [u[b][p] for b in range(4)])
            gy = combine(D_half[p], mix(a))
            return gx, gy

        @functools.cache
        def fx(a, p):
            gx, gy = flux(a, p)
            return add(
                None if gx is None else m(0, a, p) * gx, None if gy is None else m(1, a, p) * gy
            )

        @functools.cache
        def mix_fy(a):
            parts = []
            for p in range(2):
                gx, gy = flux(a, p)
                parts.append(add(
                    None if gx is None else m(1, a, p) * gx, None if gy is None else m(2, a, p) * gy
                ))
            return mixed(*parts)

        def w(a, p):
            return add(
                combine(minus_t[a], [fx(b, p) for b in range(4)]), combine(minus_half[p], mix_fy(a))
            )

        return w

    def wide(row):
        return jnp.broadcast_to(row, tile)

    def in_all_lanes(v, y):
        return jnp.broadcast_to(v[:, y:y + 1], tile)

    def tile_of(column, p):
        return jnp.where(is_low, wide(column(2 * p)), wide(column(2 * p + 1)))

    def metrics(ref, *at):
        return functools.cache(
            lambda slot, a, p: tile_of(lambda j: ref[(*at, j, pl.ds(4 * slot + a, 1))], p)
        )

    def own_metrics(ex, ey):
        return functools.cache(lambda slot, a, p: tile_of(
            lambda j: B[ex, 4 * ey + j, 4 * slot + a:4 * slot + a + 1, :], p
        ))

    def inverse_mass(x, q):
        return own_metrics(x // 4, q // 2)(3, x % 4, q % 2)

    def copy_of(group, k, src, dst):
        return pltpu.make_async_remote_copy(
            src_ref=src, dst_ref=dst, send_sem=send_sem, recv_sem=recv_sem.at[group],
            device_id=peers[k], device_id_type=MESH,
        )

    def arrived(group, landed):
        pltpu.make_async_remote_copy(
            src_ref=landed, dst_ref=landed, send_sem=send_sem, recv_sem=recv_sem.at[group],
            device_id=peers[0], device_id_type=MESH,
        ).wait_recv()

    def row_metrics(s):
        return [copy_of(3 + 3 * (1 - s), s, sM.at[s], rMr.at[1 - s])] + [
            copy_of(9 + 1 - s, 4 + 2 * s + t, sMd.at[s, t], rMd.at[1 - s, 1 - t]) for t in range(2)
        ]

    def row_edges(s, at, size):
        return copy_of(4 + 3 * (1 - s), s, sA.at[s, pl.ds(at, size)], rA.at[1 - s, pl.ds(at, size)])

    def row_corners(s):
        return [
            copy_of(
                4 + 3 * (1 - s), 4 + 2 * s + t,
                sA.at[s, pl.ds(corner_at[t], 4)], rA.at[1 - s, pl.ds(corner_at[1 - t], 4)],
            )
            for t in range(2)
        ]

    def row_parts(s):
        return copy_of(5 + 3 * (1 - s), s, sRB.at[s], rRB.at[1 - s])

    def all_to(s):
        return [*row_metrics(s), row_edges(s, 0, nq + 3), *row_corners(s), row_parts(s)]

    def start(*those):
        for copy in those:
            copy.start()

    for copy in small:
        copy.wait()
    mass = mass_ref[...]
    x_at = lax.broadcasted_iota(jnp.int32, (nx, ny), 0)
    y_at = lax.broadcasted_iota(jnp.int32, (nx, ny), 1)
    zero_row, zero_col = jnp.zeros((1, ny), jnp.float32), jnp.zeros((nx, 1), jnp.float32)
    down = jnp.concatenate([zero_row, mass[: nx - 1]], axis=0)
    up = jnp.concatenate([mass[1:], zero_row], axis=0)
    mass = mass + jnp.where((x_at & 3) == 0, down, 0.0) + jnp.where((x_at & 3) == 3, up, 0.0)
    back = jnp.concatenate([zero_col, mass[:, : ny - 1]], axis=1)
    ahead = jnp.concatenate([mass[:, 1:], zero_col], axis=1)
    mass = mass + jnp.where((y_at & 3) == 0, back, 0.0) + jnp.where((y_at & 3) == 3, ahead, 0.0)
    cross = cross_ref[...]
    for slot, v in enumerate((diag_ref[:, 0, :], cross, diag_ref[:, 1, :], mass)):
        for ex in range(nbx):
            met[ex, 4 * slot:4 * slot + 4, :ny] = v[4 * ex:4 * ex + 4]

    sub = lax.broadcasted_iota(jnp.int32, tile, 0)
    halves_of = [pl.ds(8 * i, 8) for i in range(2)]

    half_lanes = 32

    def side_by_side(v, w):
        return jnp.where(lane < half_lanes, v, pltpu.roll(w, half_lanes, 1))

    for s in range(2):
        sM[s] = side_by_side(*[met[s * (nbx - 1), half, :] for half in halves_of])
    for t in range(2):
        packed = [jnp.zeros(tile, jnp.float32)] * 2
        for ex in range(nbx):
            for i, half in enumerate(halves_of):
                v = pltpu.roll(met[ex, half, :], (4 * ex - t * (ny - 4)) % lanes, 1)
                packed[i] = jnp.where((lane >= 4 * ex) & (lane < 4 * ex + 4), v, packed[i])
        sM[2 + t] = side_by_side(*packed)
    for s in range(2):
        for t in range(2):
            y, v = t * (ny - 4), sM[s]
            v = jnp.where(
                lane < 4, pltpu.roll(v, -y % lanes, 1), pltpu.roll(v, (4 - half_lanes - y) % lanes, 1)
            )
            v = pltpu.roll(jnp.where(lane < 8, v, 0.0), 0, 1, stride=8, stride_axis=0)
            sMd[s, t] = jnp.sum(v, axis=0, keepdims=True)

    def inverted(ex, mass_of=lambda v: v):
        v = met[ex, halves_of[1], :]
        return jnp.where(sub < 4, v, 1.0 / mass_of(v))

    def lift_own(ex):
        v, w = met[ex, halves_of[0], :], inverted(ex)
        for y in range(ny):
            B[ex, y, halves_of[0], :] = in_all_lanes(v, y)
            B[ex, y, halves_of[1], :] = in_all_lanes(w, y)

    def lift(v, to, at, lane_of):
        for i, y in enumerate(lane_of):
            for h, half in enumerate(halves_of):
                to[(*at, i, half)] = in_all_lanes(v, y + h * half_lanes)

    def rows_sum(src, x, *at):
        if x % 4 == 0 and x > 0:
            return src(x, *at) + src(x - 1, *at)
        if x % 4 == 3 and x < nx - 1:
            return src(x, *at) + src(x + 1, *at)
        return src(x, *at)

    def across(line):
        for ey in range(1, nby):
            v, w = line[2 * ey - 1], line[2 * ey]
            line[2 * ey - 1], line[2 * ey] = v + high * swap(w), w + low * swap(v)
        return line

    def in_W(x, q):
        return W[x, q]

    def first_laplacian(ex):
        lift_own(ex)
        for ey in range(nby):
            w = laplace(
                [[raw[4 * ex + a, 2 * ey + p] for p in range(2)] for a in range(4)],
                own_metrics(ex, ey),
            )
            for a in range(4):
                for p in range(2):
                    W[4 * ex + a, 2 * ey + p] = w(a, p)

    def first_rows(xs):
        for x in xs:
            if x % 4 == 0 and x > 0:
                continue
            line = across([rows_sum(in_W, x, q) for q in range(nq)])
            for q in range(nq):
                T[x, q] = line[q]
                if x % 4 == 3 and x < nx - 1:
                    T[x + 1, q] = line[q]

    def inner_first(xs):
        for x in xs:
            for q in range(nq):
                v = T[x, q] * inverse_mass(x, q)
                U[x, q] = high * v if q == 0 else low * v if q == nq - 1 else v

    def known_values(ex, ey):
        return [
            [None if x in (0, nx - 1) else U[x, 2 * ey + p] for p in range(2)]
            for x in range(4 * ex, 4 * ex + 4)
        ]

    def known_parts(ex):
        edge = {0: (0, 0), nbx - 1: (1, 3)}.get(ex)
        line = [None] * nq
        for ey in range(nby):
            if edge is None and 0 < ey < nby - 1:
                continue
            w = laplace(known_values(ex, ey), own_metrics(ex, ey))
            if edge:
                line[2 * ey], line[2 * ey + 1] = w(edge[1], 0), w(edge[1], 1)
            for t, e in ((0, 0), (1, nby - 1)):
                if ey == e:
                    for a in range(4):
                        side[t, 4 * ex + a] = w(a, t)
        if edge:
            line = across(line)
            for q in range(nq):
                sRB[edge[0], q] = line[q]

    def stage_edge(s):
        for q in range(nq):
            sA[s, q] = T[s * (nx - 1), q]

    def stage_corner(s, t):
        xe, near, q = s * (nx - 1), (nx - 4 if s else 1), t * (nq - 1)
        for p in range(2):
            sA[s, corner_at[t] + p] = T[xe, t * (nq - 2) + p]
        if t == 0:
            for i in range(3):
                sA[s, nq + i] = jnp.where(is_low, T[near + i, 0], T[near + i, nq - 1])
        halves = [T[near + i, q] for i in range(3)] + [sRB[s, q]]
        for i in range(2):
            sA[s, corner_at[t] + 2 + i] = pack_column(t, halves[2 * i], halves[2 * i + 1])

    def pack_column(t, v, w):
        return jnp.where(is_low, swap(v), w) if t else jnp.where(is_low, v, swap(w))

    def exchange(first, hold=False):
        near, far = (lambda s: s * (nbx - 1)), (lambda s: 1 + s * (nbx - 3))
        rows = [range(3), range(nx - 3, nx)]
        pair = [3, nx - 5]
        edge_rows = [range(1, 4), range(nx - 4, nx - 1)]
        other = 1 - first
        columns = [copy_of(0, 2 + t, sM.at[2 + t], rMc.at[1 - t]) for t in range(2)]

        first_laplacian(near(first))
        first_rows(rows[first])
        stage_edge(first)
        if not hold:
            pl.semaphore_wait(barrier, 8 if first else jnp.where(face == 1, 5, 8))
            start(*row_metrics(first), row_edges(first, 0, nq), *columns)
            are_late, those = ((face <= 2, before), (face == faces - 1, after))[first]

            @pl.when(are_late)
            def _():
                for k in those:
                    pl.semaphore_signal(
                        late.at[1 - first], inc=1, device_id=peers[k], device_id_type=MESH
                    )

        first_laplacian(far(first))
        first_rows([pair[first]])

        def known(s):
            inner_first(edge_rows[s])
            known_parts(near(s))
            for t in range(2):
                stage_corner(s, t)

        known(first)
        if not hold:
            start(row_edges(first, nq, 3), *row_corners(first), row_parts(first))
        for ex in range(nbx):
            if ex not in (near(first), far(first)):
                first_laplacian(ex)
        first_rows(range(5, nx - 5))
        first_rows([*rows[other], pair[other]])
        if hold:
            pl.semaphore_wait(barrier, 2)
            start(*columns)
        for t in range(2):
            q = t * (nq - 1)
            for k in range(nx // 2):
                sCA[t, k] = pack_column(t, T[2 * k, q], T[2 * k + 1, q])
            for s in range(2):
                for p in range(2):
                    sCA[t, nx // 2 + 2 * s + p] = T[s * (nx - 1), t * (nq - 2) + p]
            start(copy_of(1, 2 + t, sCA.at[t], rCA.at[1 - t]))
        def to_other(*those):
            if other:
                @pl.when(face > 1)
                def _():
                    start(*those)
            elif not hold:
                start(*those)

        stage_edge(other)
        to_other(*row_metrics(other), row_edges(other, 0, nq))
        known(other)
        to_other(row_edges(other, nq, 3), *row_corners(other), row_parts(other))
        inner_first(range(4, nx - 4))
        for ex in range(1, nbx - 1):
            known_parts(ex)
        for t in range(2):
            def in_side(x, t=t):
                return side[t, x]

            for k in range(nx // 2):
                sCB[t, k] = pack_column(t, rows_sum(in_side, 2 * k), rows_sum(in_side, 2 * k + 1))
            start(copy_of(2, 2 + t, sCB.at[t], rCB.at[1 - t]))
        if other:
            @pl.when(face == 1)
            def _():
                pl.semaphore_wait(late.at[1], 3)
                start(*all_to(1))

    load.wait()

    @pl.when(face == 0)
    def _():
        exchange(1, hold=True)

    @pl.when((face > 0) & (face < faces - 1))
    def _():
        exchange(0)

    @pl.when(face >= faces - 1)
    def _():
        exchange(1)

    def turned(v, shift):
        return pltpu.roll(v, shift % lanes, 1)

    def mass_row(v, a):
        return wide(v[4 + a:5 + a, :])

    def at_ends(left, right):
        return jnp.where(lane == 0, left, 0.0) + jnp.where(lane == ny - 1, right, 0.0)

    def column_masses(t, ex):
        return turned(rMc[t], t * (ny - 1) - (half_lanes + 4 * ex + 3 * (1 - t)))

    def column_part(ref, t, x):
        v = ref[t, x // 2]
        if x % 2 != t:
            v = swap(v)
        return (high if t else low) * v

    def second_elements(ex, eys):
        for ey in eys:
            w = laplace(
                [[U[4 * ex + a, 2 * ey + p] for p in range(2)] for a in range(4)],
                own_metrics(ex, ey),
            )
            for a in range(4):
                for p in range(2):
                    W[4 * ex + a, 2 * ey + p] = w(a, p)

    def side_elements(t, ex, row=None, ext=None):
        u = []
        for a in range(4):
            v = swap(U[4 * ex + a, t * (nq - 1)])
            u.append([low * v, None] if t else [None, high * v])
        if row is not None:
            u[row] = ext
        w = laplace(u, metrics(Bc, t, ex))
        for a in range(4):
            side[t, 4 * ex + a] = w(a, 1 - t)

    inner = range(1, nby - 1)
    for ex in range(1, nbx - 1):
        second_elements(ex, inner)
    arrived(0, rMc)
    for ex in range(nbx):
        v = inverted(ex, lambda v: v + at_ends(column_masses(0, ex), column_masses(1, ex)))
        for y in (0, ny - 1):
            B[ex, y, halves_of[1], :] = in_all_lanes(v, y)
        for t in range(2):
            lift(rMc[t], Bc, (t, ex), range(4 * ex, 4 * ex + 4))
    arrived(1, rCA)
    for x in range(1, nx - 1):
        for t in range(2):
            q = t * (nq - 1)
            U[x, q] = (T[x, q] + column_part(rCA, t, x)) * inverse_mass(x, q)
    for ex in range(1, nbx - 1):
        second_elements(ex, (0, nby - 1))
        for t in range(2):
            side_elements(t, ex)

    @pl.when(face == 0)
    def _():
        pl.semaphore_wait(late.at[1], 3)
        start(*all_to(1))
        pl.semaphore_wait(late.at[0], 3)
        start(*all_to(0))

    arrived(2, rCB)

    def summed(x, halo=None, corner=None):
        line = [rows_sum(in_W, x, q) for q in range(nq)]
        if halo:
            line = [add(v, h) for v, h in zip(line, halo)]
        line = across(line)
        for t in range(2):
            q = t * (nq - 1)
            v = rows_sum(lambda x: side[t, x], x)
            if corner:
                v = v + corner[t]
            v = swap(v)
            if corner:
                last = rA[s_of(x), corner_at[t] + 3]
                v = v + (last if t else swap(last))
            line[q] = line[q] + (high if t else low) * v + column_part(rCB, t, x)
        return line

    def s_of(x):
        return 0 if x == 0 else 1

    def finish(x):
        line = summed(x)
        for at in [x] + ([x + 1] if x % 4 == 3 and x < nx - 1 else []):
            for q in range(nq):
                out_ref[at, q] = line[q] * inverse_mass(at, q)

    for x in range(5, nx - 5):
        if x % 4:
            finish(x)

    def ring_metrics(s):
        ex, own_row, halo_row = s * (nbx - 1), 3 * s, 3 - 3 * s
        arrived(3 + 3 * s, rMr.at[s])
        arrived(9 + s, rMd.at[s])
        theirs = [rMr[s]]
        for t in range(2):
            y = (1 - t) * (ny - 4)
            row = wide(rMd[s, t])
            v = row
            for i in range(1, 8):
                v = jnp.where(sub == i, turned(row, -8 * i), v)
            theirs.append(jnp.where(
                lane < half_lanes, turned(v, y), turned(v, half_lanes + y - 4)
            ))
        beyond = [turned(v, -half_lanes) for v in theirs]
        own = sub == 4 + own_row
        ends = [
            column_masses(t, ex)
            + jnp.where(own, mass_row(turned(beyond[1 + t], (2 * t - 1) * (ny - 1)), halo_row), 0.0)
            for t in range(2)
        ]
        v = inverted(ex, lambda v: (
            v + jnp.where(own, mass_row(beyond[0], halo_row), 0.0) + at_ends(*ends)
        ))
        for y in range(ny):
            B[ex, y, halves_of[1], :] = in_all_lanes(v, y)
        lift(theirs[0], Br, (s,), range(ny))
        for t in range(2):
            lift(theirs[1 + t], Bd, (2 * s + t,), range(4) if t else range(ny - 4, ny))
            v = 1.0 / (
                mass_row(turned(rMc[t], -(half_lanes + 4 * ex)), own_row)
                + mass_row(turned(beyond[1 + t], 0 if t else -(ny - 4)), halo_row)
            )
            for p in range(2):
                inv[s, 2 * t + p] = jnp.where(
                    is_low, in_all_lanes(v, 2 * p), in_all_lanes(v, 2 * p + 1)
                )
        v = 1.0 / (beyond[0] + at_ends(
            turned(beyond[1], -(ny - 1)), turned(beyond[2], ny - 1)
        ))
        for i in range(3):
            row = mass_row(v, i + s)
            inv[s, 4 + i] = jnp.where(is_low, in_all_lanes(row, 0), in_all_lanes(row, ny - 1))

    def ring_rows(s):
        xe, ex, own_row, halo_row = s * (nx - 1), s * (nbx - 1), 3 * s, 3 - 3 * s
        rest = [a for a in range(4) if a != halo_row]
        arrived(4 + 3 * s, rA.at[s])
        for q in range(nq):
            v = T[xe, q] + rA[s, q]
            for t in range(2):
                if q == t * (nq - 1):
                    v = v + column_part(rCA, t, xe)
                    v = v + (high if t else low) * swap(rA[s, corner_at[t] + 1 - t])
            U[xe, q] = v * inverse_mass(xe, q)
        ext = []
        for t in range(2):
            e = [
                (rCA[t, nx // 2 + 2 * s + p] + rA[s, corner_at[t] + p]) * inv[s, 2 * t + p]
                for p in range(2)
            ]
            corner = swap(U[xe, t * (nq - 1)])
            e[1 - t] = high * e[0] + low * corner if t else low * e[1] + high * corner
            ext.append(e)
        beyond = []
        for i in range(3):
            v, w = [rA[s, at + 2 + i // 2] for at in corner_at]
            v, w = (swap(v), w) if i % 2 else (v, swap(w))
            beyond.append((rA[s, nq + i] + low * v + high * w) * inv[s, 4 + i])

        second_elements(ex, range(nby))
        for t in range(2):
            side_elements(t, ex, own_row, ext[t])
        halo = []
        for ey in range(nby):
            u = [[None, None] for _ in range(4)]
            u[halo_row] = [U[xe, 2 * ey + p] for p in range(2)]
            for i, a in enumerate(rest):
                if ey == 0:
                    u[a][0] = low * beyond[i]
                if ey == nby - 1:
                    u[a][1] = high * beyond[i]
            w = laplace(u, functools.cache(lambda slot, a, p, ey=ey: tile_of(
                lambda j: Br[s, 4 * ey + j, 4 * slot + a:4 * slot + a + 1, :], p
            )))
            halo += [w(halo_row, 0), w(halo_row, 1)]
        corner = []
        for t in range(2):
            u = [[None, None] for _ in range(4)]
            u[halo_row] = ext[t]
            for i, a in enumerate(rest):
                v = swap(beyond[i])
                u[a] = [low * v, None] if t else [None, high * v]
            w = laplace(u, metrics(Bd, 2 * s + t))
            corner.append(w(halo_row, 1 - t))
        for x in (range(nx - 5, nx) if s else range(5)):
            if x % 4 and x != xe:
                finish(x)
        line = summed(xe, halo, corner)
        for q in range(nq):
            T[xe, q] = line[q]

    def last_row(s):
        xe = s * (nx - 1)
        arrived(5 + 3 * s, rRB.at[s])
        for q in range(nq):
            out_ref[xe, q] = (T[xe, q] + rRB[s, q]) * inverse_mass(xe, q)


    ring_metrics(1)

    @pl.when(face != 0)
    def _():
        ring_metrics(0)

    ring_rows(1)

    @pl.when(face == 0)
    def _():
        ring_metrics(0)

    ring_rows(0)
    last_row(1)
    last_row(0)
    pltpu.make_async_remote_copy(
        src_ref=sent, dst_ref=sent, send_sem=send_sem, recv_sem=recv_sem.at[0],
        device_id=peers[0], device_id_type=MESH,
    ).wait_send()


def solution(mesh):
    faces, cols = mesh.shape["face"], mesh.shape["col"]

    def shards(fields, metric_diag, metric_cross, point_mass):
        nf, nx, ny, lanes = fields.shape
        nbx, nby = nx // 4, ny // 4
        nq = ny // 2
        f32 = jnp.float32
        tiles = (nx, nq, 2 * nf, lanes)

        def vmem(*shape):
            return pltpu.VMEM(shape, f32)

        def messages():
            return [
                vmem(2, nq + 3 + 8, 2 * nf, lanes),
                vmem(2, nq, 2 * nf, lanes),
                vmem(2, nx // 2 + 4, 2 * nf, lanes),
                vmem(2, nx // 2, 2 * nf, lanes),
            ]

        tiles_sent = 2 * (2 * nq + 3 + 4) + 2 * (nx + 4) + 8 + 4
        out = pl.pallas_call(
            functools.partial(kernel, faces, cols, nf, nbx, nby),
            out_shape=jax.ShapeDtypeStruct(tiles, f32),
            in_specs=[pl.BlockSpec(memory_space=pltpu.HBM)] * 4,
            out_specs=pl.BlockSpec(memory_space=pltpu.VMEM),
            scratch_shapes=[
                vmem(nx, 2, ny),
                vmem(nx, ny),
                vmem(nx, ny),
                vmem(*tiles),
                vmem(*tiles),
                vmem(*tiles),
                vmem(*tiles),
                vmem(2, nx, 2 * nf, lanes),
                vmem(nbx, 16, lanes),
                vmem(nbx, ny, 16, lanes),
                vmem(2, ny, 16, lanes),
                vmem(2, nbx, 4, 16, lanes),
                vmem(4, 4, 16, lanes),
                vmem(2, 7, 2 * nf, lanes),
                vmem(4, 2 * nf, lanes),
                vmem(2, 2, 1, lanes),
                *messages(),
                vmem(2, 2 * nf, lanes),
                vmem(2, 2 * nf, lanes),
                vmem(2, 2, 1, lanes),
                *messages(),
                vmem(tiles_sent * 2 * nf + 4, 1, lanes),
                pltpu.SemaphoreType.DMA((3,)),
                pltpu.SemaphoreType.DMA,
                pltpu.SemaphoreType.DMA,
                pltpu.SemaphoreType.DMA((11,)),
                pltpu.SemaphoreType.REGULAR((2,)),
            ],
            compiler_params=pltpu.CompilerParams(
                collective_id=0, has_side_effects=True, vmem_limit_bytes=32 * 1024 * 1024
            ),
        )(*[
            pltpu.with_memory_space_constraint(v, pltpu.HBM)
            for v in (
                fields.transpose(1, 2, 0, 3).reshape(tiles),
                metric_diag.transpose(1, 0, 2), metric_cross, point_mass,
            )
        ])
        return out.reshape(nx, ny, nf, lanes).transpose(2, 0, 1, 3)

    return jax.shard_map(
        shards,
        mesh=mesh,
        in_specs=(
            P(None, "face", "col", None),
            P(None, "face", "col"),
            P("face", "col"),
            P("face", "col"),
        ),
        out_specs=P(None, "face", "col", None),
        check_vma=False,
    )
```
